8 devices in a mesh: dp: 2 (over z, y), tp: 4 (over x, core).
Axes of the slice: x: 2, y: 2, z: 1, core: 2. Of those that a mesh axis runs over, the one named last changes fastest.
Arguments:
- x_in: float32 [8, 128, 2048], P('dp', 'tp'), parts along dimension 0
- d_out: bfloat16 [8, 128, 2048], P('dp', 'tp'), parts along dimension 0
- lengths: int32 [8], P('dp'), parts along dimension 0
- w_qkv: bfloat16 [4, 2048, 3, 32, 64], P(None, None, None, 'tp')
- w_out: bfloat16 [4, 32, 64, 2048], P(None, 'tp')
- w_up: bfloat16 [4, 2048, 8192], P(None, None, 'tp')
- b_up: float32 [4, 8192], P(None, 'tp')
- w_down: bfloat16 [4, 8192, 2048], P(None, 'tp')
- vec_par: float32 [4, 6, 2048], replicated
Outputs:
- output 1: float32 [8, 128, 2048], P('dp', 'tp'), parts along dimension 0
- output 2: float32 [8, 128, 2048], P('dp', 'tp'), parts along dimension 0
- output 3: bfloat16 [8, 2048, 3, 32, 64], P('dp', None, None, 'tp'), parts along dimension 0
- output 4: bfloat16 [8, 32, 64, 2048], P('dp', 'tp'), parts along dimension 0
- output 5: bfloat16 [8, 2048, 8192], P('dp', None, 'tp'), parts along dimension 0
- output 6: float32 [8, 8192], P('dp', 'tp'), parts along dimension 0
- output 7: bfloat16 [8, 8192, 2048], P('dp', 'tp'), parts along dimension 0
- output 8: float32 [8, 6, 2048], P('dp'), parts along dimension 0
There are 2 independent parts. The reference program is written for one: setup_inputs(seed, part) draws one part's arguments, and reference() takes and returns one part's arrays. A program takes and returns all parts, laid end to end along the dimension named above; an argument that names none is the same for every part.
All inputs are finite; a program needn't handle non-finite values.
Results may differ from the reference program's by a relative error of at most 0.02.
Values are sent between devices in bfloat16 or wider.
A program may use at most 1 GiB of HBM per device.

```python
import functools
import jax
import jax.numpy as jnp
from jax import lax

BATCH_GROUP = 4
SEQ_LEN = 128
D_MODEL = 2048
NUM_HEADS = 32
HEAD_DIM = 64
FF_DIM = 8192
LAYERS = 4


def draw_lengths(key_len, key_perm):
    lengths = jax.random.randint(key_len, (BATCH_GROUP,), SEQ_LEN // 4, SEQ_LEN + 1, jnp.int32)
    perm_order = jax.random.permutation(key_perm, BATCH_GROUP)
    return lengths.at[perm_order[0]].set(SEQ_LEN).at[perm_order[1]].set(SEQ_LEN // 4)


def setup_inputs(seed: int = 0, part: int = 0) -> dict:
    shared_key = jax.random.key(seed)
    part_key = jax.random.fold_in(jax.random.key(seed + 1), part)
    key_qkv, key_out, key_up, key_bup, key_down, key_vec = jax.random.split(shared_key, 6)
    key_x, key_dy, key_len, key_perm = jax.random.split(part_key, 4)
    inner_dim = NUM_HEADS * HEAD_DIM
    w_qkv = (jax.random.normal(key_qkv, (LAYERS, D_MODEL, 3, NUM_HEADS, HEAD_DIM), jnp.float32) * (1.2 * D_MODEL ** -0.5)).astype(jnp.bfloat16)
    w_out = (jax.random.normal(key_out, (LAYERS, NUM_HEADS, HEAD_DIM, D_MODEL), jnp.float32) * (2.0 * inner_dim ** -0.5)).astype(jnp.bfloat16)
    w_up = (jax.random.normal(key_up, (LAYERS, D_MODEL, FF_DIM), jnp.float32) * D_MODEL ** -0.5).astype(jnp.bfloat16)
    b_up = jax.random.normal(key_bup, (LAYERS, FF_DIM), jnp.float32) * 0.5
    w_down = (jax.random.normal(key_down, (LAYERS, FF_DIM, D_MODEL), jnp.float32) * (2.0 * FF_DIM ** -0.5)).astype(jnp.bfloat16)
    row_scale = jnp.array([0.25, 0.5, 0.25, 0.5, 0.5, 0.5], jnp.float32)[None, :, None]
    row_base = jnp.array([1.0, 0.0, 1.0, 0.0, 0.0, 0.0], jnp.float32)[None, :, None]
    vec_par = jax.random.normal(key_vec, (LAYERS, 6, D_MODEL), jnp.float32) * row_scale + row_base
    x_in = jax.random.normal(key_x, (BATCH_GROUP, SEQ_LEN, D_MODEL), jnp.float32)
    d_out = jax.random.normal(key_dy, (BATCH_GROUP, SEQ_LEN, D_MODEL), jnp.float32).astype(jnp.bfloat16)
    lengths = draw_lengths(key_len, key_perm)
    return {'x_in': x_in, 'd_out': d_out, 'lengths': lengths, 'w_qkv': w_qkv, 'w_out': w_out, 'w_up': w_up, 'b_up': b_up, 'w_down': w_down, 'vec_par': vec_par}


def layer_norm(x_val, gain_vec, shift_vec):
    row_mean = jnp.mean(x_val, axis=-1, keepdims=True)
    centered = x_val - row_mean
    row_var = jnp.mean(centered * centered, axis=-1, keepdims=True)
    return centered * lax.rsqrt(row_var + 1e-5) * gain_vec + shift_vec


def attend_one(item_tuple):
    q_one, k_one, v_one, length = item_tuple
    scores = jnp.einsum('hqe,hke->hqk', q_one.astype(jnp.float32), k_one.astype(jnp.float32)) * HEAD_DIM ** -0.5
    positions = jnp.arange(SEQ_LEN)
    allowed = (positions[None, :] <= positions[:, None]) & (positions[None, :] < length)
    scores = jnp.where(allowed[None], scores, -1e30)
    attn_prob = jax.nn.softmax(scores, axis=-1).astype(jnp.bfloat16)
    context = jnp.einsum('hqk,hke->hqe', attn_prob.astype(jnp.float32), v_one.astype(jnp.float32))
    return context.astype(jnp.bfloat16)


def gpt_layer(x_val, layer_par, lengths):
    w_qkv, w_out, w_up, b_up, w_down, vec_layer = layer_par
    a_in = layer_norm(x_val, vec_layer[0], vec_layer[1]).astype(jnp.bfloat16)
    qkv_all = jnp.einsum('bsd,dthe->tbhse', a_in.astype(jnp.float32), w_qkv.astype(jnp.float32)).astype(jnp.bfloat16)
    context = lax.map(attend_one, (qkv_all[0], qkv_all[1], qkv_all[2], lengths))
    attn_out = jnp.einsum('bhse,hed->bsd', context.astype(jnp.float32), w_out.astype(jnp.float32)).astype(jnp.bfloat16)
    hidden = x_val + attn_out.astype(jnp.float32) + vec_layer[4]
    a_mid = layer_norm(hidden, vec_layer[2], vec_layer[3]).astype(jnp.bfloat16)
    pre_act = jnp.einsum('bsd,df->bsf', a_mid.astype(jnp.float32), w_up.astype(jnp.float32)) + b_up
    act_bf = jax.nn.gelu(pre_act, approximate=True).astype(jnp.bfloat16)
    mlp_out = jnp.einsum('bsf,fd->bsd', act_bf.astype(jnp.float32), w_down.astype(jnp.float32)).astype(jnp.bfloat16)
    return hidden + mlp_out.astype(jnp.float32) + vec_layer[5]


def forward_stack(x_in, w_qkv, w_out, w_up, b_up, w_down, vec_par, lengths):
    def scan_step(carry_x, layer_par):
        return gpt_layer(carry_x, layer_par, lengths), None
    return lax.scan(scan_step, x_in, (w_qkv, w_out, w_up, b_up, w_down, vec_par))[0]


def reference(x_in, d_out, lengths, w_qkv, w_out, w_up, b_up, w_down, vec_par):
    y_out, pullback = jax.vjp(functools.partial(forward_stack, lengths=lengths), x_in, w_qkv, w_out, w_up, b_up, w_down, vec_par)
    grad_list = pullback(d_out.astype(jnp.float32))
    return (y_out, grad_list[0], grad_list[1], grad_list[2], grad_list[3], grad_list[4], grad_list[5], grad_list[6])
```

```python
import functools
import jax
import jax.numpy as jnp
from jax import lax
from jax.experimental import pallas as pl
from jax.experimental.pallas import tpu as pltpu
from jax.sharding import PartitionSpec as P

TENSOR_AXIS = 'tp'
PARTS_AXIS = 'dp'
BF = jnp.bfloat16
F32 = jnp.float32
MESH = pl.DeviceIdType.MESH
VMEM_LIMIT = 67043328
NUM_CHUNKS = 2
RS_BLOCKS = 2
GELU_C = 0.7978845608028654


def dot_nn(a, b):
    return lax.dot_general(a, b, (((1,), (0,)), ((), ())), preferred_element_type=F32)


def dot_nt(a, b):
    return lax.dot_general(a, b, (((1,), (1,)), ((), ())), preferred_element_type=F32)


def dot_tn(a, b):
    return lax.dot_general(a, b, (((0,), (0,)), ((), ())), preferred_element_type=F32)


def seqs(c):
    return pl.ds(2 * c, 2)


def slab(r):
    return pl.ds(32 * r, 32)


def rows_of(ref, c):
    val = ref[seqs(c)]
    return val.reshape(256, val.shape[-1])


def normed(z):
    mean = jnp.mean(z, axis=-1, keepdims=True)
    centered = z - mean
    var = jnp.mean(centered * centered, axis=-1, keepdims=True)
    rstd = lax.rsqrt(var + 1e-5)
    return centered * rstd, rstd


class Exchange:
    def __init__(self, part, from_core, far_send, far_recv, sems):
        self.me = lax.axis_index(TENSOR_AXIS)
        self.part, self.from_core = part, from_core
        self.far_send, self.far_recv = far_send, far_recv
        self.gs, self.gr, self.cs, self.cr, self.xs, self.xr = sems

    def remote(self, src, dst, send, recv, flip):
        return pltpu.make_async_remote_copy(
            src_ref=src, dst_ref=dst, send_sem=send, recv_sem=recv,
            device_id={TENSOR_AXIS: lax.bitwise_xor(self.me, flip)}, device_id_type=MESH)

    def barrier(self):
        sem = pltpu.get_barrier_semaphore()
        for flip in (1, 2):
            pl.semaphore_signal(sem, inc=1, device_id={TENSOR_AXIS: lax.bitwise_xor(self.me, flip)}, device_id_type=MESH)
        pl.semaphore_wait(sem, 2)

    def gather_copy(self, buf, c, which):
        src, dst, flip = ((0, 2, 2), (0, 1, 1), (2, 3, 1))[which]
        return self.remote(buf.at[seqs(c), slab(src)], buf.at[seqs(c), slab(dst)], self.gs.at[c, which], self.gr.at[c, which], flip)

    def gather_start(self, buf, c):
        self.gather_copy(buf, c, 0).start()
        self.gather_copy(buf, c, 1).start()

    def gather_finish(self, buf, c):
        self.gather_copy(buf, c, 0).wait_recv()
        self.gather_copy(buf, c, 2).start()
        self.gather_copy(buf, c, 1).wait_recv()
        self.gather_copy(buf, c, 2).wait_recv()
        for which in range(3):
            self.gather_copy(buf, c, which).wait_send()

    def cols(self, b):
        width = self.part.shape[-1] // RS_BLOCKS
        return pl.ds(b * width, width)

    def core_copy(self, c, b, which):
        return self.remote(self.part.at[seqs(c), slab((1, 3)[which]), self.cols(b)],
                           self.from_core.at[seqs(c), slab(which), self.cols(b)],
                           self.cs.at[c, b, which], self.cr.at[c, b, which], 1)

    def far_copy(self, c, b):
        return self.remote(self.far_send.at[seqs(c), :, self.cols(b)], self.far_recv.at[seqs(c), :, self.cols(b)],
                           self.xs.at[c, b], self.xr.at[c, b], 2)

    def scatter_start(self, c, b):
        self.core_copy(c, b, 1).start()
        self.core_copy(c, b, 0).start()

    def scatter_middle(self, c, b):
        self.core_copy(c, b, 1).wait_recv()
        near = self.part[seqs(c), slab(2), self.cols(b)].astype(F32)
        self.far_send[seqs(c), :, self.cols(b)] = (near + self.from_core[seqs(c), slab(1), self.cols(b)].astype(F32)).astype(BF)
        self.far_copy(c, b).start()

    def scatter_finish(self, c):
        for b in range(RS_BLOCKS):
            self.core_copy(c, b, 0).wait_recv()
            self.far_copy(c, b).wait_recv()
            self.core_copy(c, b, 0).wait_send()
            self.core_copy(c, b, 1).wait_send()
            self.far_copy(c, b).wait_send()
        total = self.part[seqs(c), slab(0)].astype(F32) + self.from_core[seqs(c), slab(0)].astype(F32)
        return (total + self.far_recv[seqs(c)].astype(F32)).astype(BF).astype(F32)

    @staticmethod
    def scratch(d):
        dma = pltpu.SemaphoreType.DMA
        return [pltpu.VMEM((4, 128, d), BF), pltpu.VMEM((4, 64, d), BF), pltpu.VMEM((4, 32, d), BF), pltpu.VMEM((4, 32, d), BF),
                dma((2, 3)), dma((2, 3)), dma((2, RS_BLOCKS, 2)), dma((2, RS_BLOCKS, 2)), dma((2, RS_BLOCKS)), dma((2, RS_BLOCKS))]


def partial_sum(ex, c, block_of, bn=512):
    width = ex.part.shape[-1] // RS_BLOCKS
    for b in range(RS_BLOCKS):
        for j in range(width // bn):
            cols = pl.ds(b * width + j * bn, bn)
            ex.part[seqs(c), :, cols] = block_of(cols).astype(BF).reshape(2, 128, bn)
        ex.scatter_start(c, b)


def lane_low():
    return lax.broadcasted_iota(jnp.int32, (128, 128), 1) < 64


def two_heads(val, low):
    zero = jnp.zeros_like(val)
    return jnp.concatenate([jnp.where(low, val, zero), jnp.where(low, zero, val)], axis=0)


def forward_kernel(x_in, mask, vec, bup, wqkv_h, wout_h, wup_h, wdown_h,
                   y_out, x_s, hid_s, a_s, qkv_s, ctx_s, p_s, m_s, u_s, act_s,
                   wq, wo, wu, wd, xbuf, hbuf, ag_a, ag_m, qkv, ctx, prob, u, act,
                   wsem, ssem, part, from_core, far_send, far_recv, *sems):
    n_layers = wqkv_h.shape[0]
    ex = Exchange(part, from_core, far_send, far_recv, sems)

    def weight_copies(l, kind):
        pairs = ((wqkv_h, wq, 0), (wout_h, wo, 1)) if kind == 0 else ((wup_h, wu, 2), (wdown_h, wd, 3))
        return [pltpu.make_async_copy(src.at[l], dst, wsem.at[i]) for src, dst, i in pairs]

    def save_copies(l, c, kind):
        if kind == 0:
            pairs = ((xbuf, x_s, 0), (ag_a, a_s, 1), (qkv, qkv_s, 2), (ctx, ctx_s, 3), (prob, p_s, 4))
        else:
            pairs = ((hbuf, hid_s, 5), (ag_m, m_s, 6), (u, u_s, 7), (act, act_s, 8))
        return [pltpu.make_async_copy(src.at[seqs(c)], dst.at[l, seqs(c)], ssem.at[c, i]) for src, dst, i in pairs]

    def norm_and_send(src, l, c, row, buf):
        xhat, _ = normed(src[seqs(c)].reshape(64, -1))
        val = xhat * vec[row, pl.ds(l, 1), :] + vec[row + 1, pl.ds(l, 1), :]
        buf[seqs(c), slab(0)] = val.astype(BF).reshape(2, 32, -1)
        ex.gather_start(buf, c)

    def attention(c):
        a = rows_of(ag_a, c)
        for j in range(3):
            cols = pl.ds(512 * j, 512)
            qkv[seqs(c), :, cols] = dot_nt(a, wq[cols, :]).astype(BF).reshape(2, 128, 512)
        low = lane_low()
        for s in range(2):
            seq = 2 * c + s
            visible = mask[seq] > 0
            visible = jnp.concatenate([visible, visible], axis=0)
            for pair in range(4):
                q, k, v = (qkv[seq, :, pl.ds(512 * t + 128 * pair, 128)] for t in range(3))
                scores = dot_nt(two_heads(q, low), k) * 0.125
                scores = jnp.where(visible, scores, -1e30)
                e = jnp.exp(scores - jnp.max(scores, axis=-1, keepdims=True))
                p = e / jnp.sum(e, axis=-1, keepdims=True)
                prob[seq, pair] = p
                pb = p.astype(BF)
                both = jnp.concatenate([pb[:128], pb[128:]], axis=1)
                ctx[seq, :, pl.ds(128 * pair, 128)] = dot_nn(both, two_heads(v, low)).astype(BF)

    def mlp(l, c):
        m = rows_of(ag_m, c)

        @pl.loop(0, 4)
        def _(j):
            cols = pl.ds(pl.multiple_of(512 * j, 512), 512)
            pre = dot_nn(m, wu[:, cols]) + bup[pl.ds(l, 1), cols]
            u[seqs(c), :, cols] = pre.reshape(2, 128, 512)
            t = jnp.tanh(GELU_C * (pre + 0.044715 * (pre * pre * pre)))
            act[seqs(c), :, cols] = (0.5 * pre * (1.0 + t)).astype(BF).reshape(2, 128, 512)

    for kind in range(2):
        for copy in weight_copies(0, kind):
            copy.start()
    xbuf[...] = x_in[...]
    ex.barrier()
    for c in range(NUM_CHUNKS):
        norm_and_send(xbuf, 0, c, 0, ag_a)

    @pl.loop(0, n_layers)
    def _(l):
        for copy in weight_copies(l, 0):
            copy.wait()
        for c in range(NUM_CHUNKS):
            ex.gather_finish(ag_a, c)
            attention(c)
            for copy in save_copies(l, c, 0):
                copy.start()
            lhs = rows_of(ctx, c)
            partial_sum(ex, c, lambda cols: dot_nn(lhs, wo[:, cols]))
            for b in range(RS_BLOCKS):
                ex.scatter_middle(c, b)

        @pl.when(l + 1 < n_layers)
        def _():
            for copy in weight_copies(l + 1, 0):
                copy.start()

        for c in range(NUM_CHUNKS):
            hbuf[seqs(c)] = xbuf[seqs(c)] + ex.scatter_finish(c) + vec[4, pl.ds(l, 1), :][None]
            norm_and_send(hbuf, l, c, 2, ag_m)
        for copy in weight_copies(l, 1):
            copy.wait()
        for c in range(NUM_CHUNKS):
            ex.gather_finish(ag_m, c)
            mlp(l, c)
            for copy in save_copies(l, c, 1):
                copy.start()
            for copy in save_copies(l, c, 0):
                copy.wait()
            lhs = rows_of(act, c)
            partial_sum(ex, c, lambda cols: dot_nn(lhs, wd[:, cols]))
            for b in range(RS_BLOCKS):
                ex.scatter_middle(c, b)

        @pl.when(l + 1 < n_layers)
        def _():
            for copy in weight_copies(l + 1, 1):
                copy.start()

        for c in range(NUM_CHUNKS):
            xbuf[seqs(c)] = hbuf[seqs(c)] + ex.scatter_finish(c) + vec[5, pl.ds(l, 1), :][None]

            @pl.when(l + 1 < n_layers)
            def _():
                norm_and_send(xbuf, l + 1, c, 0, ag_a)

        for c in range(NUM_CHUNKS):
            for copy in save_copies(l, c, 1):
                copy.wait()

    y_out[...] = xbuf[...]


def backward_kernel(dy_in, vec, wqkv_h, wout_h, wup_h, wdown_h, x_s, hid_s, qkv_s, p_s, u_s,
                    d_x, dmlp_s, dpre_s, dattn_s, dqkv_s, g_bup, g_vec,
                    wq, wo, wu, wd, dcur, dhid, xbuf, hbuf, ag_a, ag_m, qkv, prob, u, dpre, dctx, dqkv, vacc, vfar,
                    wsem, rsem, ssem, vsem, part, from_core, far_send, far_recv, *sems):
    n_layers = wqkv_h.shape[0]
    ex = Exchange(part, from_core, far_send, far_recv, sems)

    def loads(l, kind):
        if kind == 0:
            whole = ((wqkv_h, wq, 0), (wout_h, wo, 1))
            saved = ((x_s, xbuf, 0), (qkv_s, qkv, 1), (p_s, prob, 2))
        else:
            whole = ((wdown_h, wd, 3), (wup_h, wu, 2))
            saved = ((u_s, u, 4), (hid_s, hbuf, 3))
        return ([pltpu.make_async_copy(src.at[l], dst, wsem.at[i]) for src, dst, i in whole]
                + [pltpu.make_async_copy(src.at[l], dst, rsem.at[i]) for src, dst, i in saved])

    def save_copies(l, c, kind):
        pairs = ((ag_a, dattn_s, 0), (dqkv, dqkv_s, 1)) if kind == 0 else ((ag_m, dmlp_s, 2), (dpre, dpre_s, 3))
        return [pltpu.make_async_copy(src.at[seqs(c)], dst.at[l, seqs(c)], ssem.at[c, i]) for src, dst, i in pairs]

    def send(src, c, buf):
        buf[seqs(c), slab(0)] = src[seqs(c)].astype(BF)
        ex.gather_start(buf, c)

    def add_row(i, l, c, val):
        row = (i, pl.ds(l, 1))
        total = jnp.sum(val, axis=0, keepdims=True)
        vacc[row] = total if c == 0 else vacc[row] + total

    def norm_bwd(z_ref, d_z, l, c, row):
        xhat, rstd = normed(z_ref[seqs(c)].reshape(64, -1))
        add_row(row, l, c, d_z * xhat)
        add_row(row + 1, l, c, d_z)
        g = d_z * vec[row, pl.ds(l, 1), :]
        g_mean = jnp.mean(g, axis=-1, keepdims=True)
        gx_mean = jnp.mean(g * xhat, axis=-1, keepdims=True)
        return rstd * (g - g_mean - xhat * gx_mean)

    def mlp_bwd(l, c):
        d_mlp = rows_of(ag_m, c)

        @pl.loop(0, 4)
        def _(j):
            cols = pl.ds(pl.multiple_of(512 * j, 512), 512)
            d_act = dot_nt(d_mlp, wd[cols, :]).astype(BF).astype(F32)
            pre = u[seqs(c), :, cols].reshape(256, 512)
            sq = pre * pre
            t = jnp.tanh(GELU_C * (pre + 0.044715 * (sq * pre)))
            slope = 0.5 * (1.0 + t) + 0.5 * pre * (1.0 - t * t) * (GELU_C * (1.0 + 0.134145 * sq))
            d_pre = d_act * slope
            total = jnp.sum(d_pre, axis=0, keepdims=True)
            g_bup[pl.ds(l, 1), cols] = total if c == 0 else g_bup[pl.ds(l, 1), cols] + total
            dpre[seqs(c), :, cols] = d_pre.astype(BF).reshape(2, 128, 512)

    def attention_bwd(c):
        dctx[seqs(c)] = dot_nt(rows_of(ag_a, c), wo[...]).astype(BF).reshape(2, 128, 512)
        low = lane_low()
        for s in range(2):
            seq = 2 * c + s
            for pair in range(4):
                q, k, v = (qkv[seq, :, pl.ds(512 * t + 128 * pair, 128)] for t in range(3))
                d_c = two_heads(dctx[seq, :, pl.ds(128 * pair, 128)], low)
                p = prob[seq, pair]
                d_p = dot_nt(d_c, v).astype(BF).astype(F32)
                d_s = p * (d_p - jnp.sum(d_p * p, axis=-1, keepdims=True))
                d_s = (d_s * 0.125).astype(BF)
                both = jnp.concatenate([d_s[:128], d_s[128:]], axis=1)
                d_q = dot_nn(both, two_heads(k, low))
                d_k = dot_tn(d_s, two_heads(q, low))
                d_v = dot_tn(p.astype(BF), d_c)
                for t, val in enumerate((d_q, d_k, d_v)):
                    dqkv[seq, :, pl.ds(512 * t + 128 * pair, 128)] = val.astype(BF)

    for kind in (1, 0):
        for copy in loads(n_layers - 1, kind):
            copy.start()
    dcur[...] = dy_in[...].astype(F32)
    ex.barrier()
    for c in range(NUM_CHUNKS):
        send(dcur, c, ag_m)

    @pl.loop(0, n_layers)
    def _(i):
        l = n_layers - 1 - i
        for copy in loads(l, 1):
            copy.wait()
        for c in range(NUM_CHUNKS):
            ex.gather_finish(ag_m, c)
            mlp_bwd(l, c)
            for copy in save_copies(l, c, 1):
                copy.start()
            lhs = rows_of(dpre, c)
            partial_sum(ex, c, lambda cols: dot_nt(lhs, wu[cols, :]))
            for b in range(RS_BLOCKS):
                ex.scatter_middle(c, b)
        for c in range(NUM_CHUNKS):
            d_cur = dcur[seqs(c)].reshape(64, -1)
            d_hid = d_cur + norm_bwd(hbuf, ex.scatter_finish(c).reshape(64, -1), l, c, 2)
            dhid[seqs(c)] = d_hid.reshape(2, 32, -1)
            send(dhid, c, ag_a)
            add_row(5, l, c, d_cur)
            add_row(4, l, c, d_hid)

        @pl.when(l > 0)
        def _():
            for copy in loads(l - 1, 1):
                copy.start()

        for copy in loads(l, 0):
            copy.wait()
        for c in range(NUM_CHUNKS):
            ex.gather_finish(ag_a, c)
            attention_bwd(c)
            for copy in save_copies(l, c, 0):
                copy.start()
            for copy in save_copies(l, c, 1):
                copy.wait()
            lhs = rows_of(dqkv, c)
            partial_sum(ex, c, lambda cols: dot_nn(lhs, wq[:, cols]))
            for b in range(RS_BLOCKS):
                ex.scatter_middle(c, b)
        for c in range(NUM_CHUNKS):
            d_ln = norm_bwd(xbuf, ex.scatter_finish(c).reshape(64, -1), l, c, 0)
            dcur[seqs(c)] = dhid[seqs(c)] + d_ln.reshape(2, 32, -1)

            @pl.when(l > 0)
            def _():
                send(dcur, c, ag_m)

        @pl.when(l > 0)
        def _():
            for copy in loads(l - 1, 0):
                copy.start()

        for c in range(NUM_CHUNKS):
            for copy in save_copies(l, c, 0):
                copy.wait()

    d_x[...] = dcur[...]
    for step, flip in enumerate((1, 2)):
        copy = ex.remote(vacc if step == 0 else g_vec, vfar.at[step], vsem.at[step, 0], vsem.at[step, 1], flip)
        copy.start()
        copy.wait()
        g_vec[...] = (vacc if step == 0 else g_vec)[...] + vfar[step]


def any_spec():
    return pl.BlockSpec(memory_space=pl.ANY)


def vmem_spec():
    return pl.BlockSpec(memory_space=pltpu.VMEM)


def run_forward(x, mask, vec, bup, wqkv, wout, wup, wdown):
    n, d = wqkv.shape[0], x.shape[-1]
    shape = jax.ShapeDtypeStruct
    dma = pltpu.SemaphoreType.DMA
    outs = [shape((4, 32, d), F32), shape((n, 4, 32, d), F32), shape((n, 4, 32, d), F32), shape((n, 4, 128, d), BF),
            shape((n, 4, 128, 1536), BF), shape((n, 4, 128, 512), BF), shape((n, 4, 4, 256, 128), F32),
            shape((n, 4, 128, d), BF), shape((n, 4, 128, d), F32), shape((n, 4, 128, d), BF)]
    return pl.pallas_call(
        forward_kernel,
        in_specs=[vmem_spec()] * 4 + [any_spec()] * 4,
        out_specs=[vmem_spec()] + [any_spec()] * 9,
        out_shape=outs,
        scratch_shapes=[pltpu.VMEM((1536, d), BF), pltpu.VMEM((512, d), BF), pltpu.VMEM((d, d), BF), pltpu.VMEM((d, d), BF),
                        pltpu.VMEM((4, 32, d), F32), pltpu.VMEM((4, 32, d), F32), pltpu.VMEM((4, 128, d), BF), pltpu.VMEM((4, 128, d), BF),
                        pltpu.VMEM((4, 128, 1536), BF), pltpu.VMEM((4, 128, 512), BF), pltpu.VMEM((4, 4, 256, 128), F32),
                        pltpu.VMEM((4, 128, d), F32), pltpu.VMEM((4, 128, d), BF), dma((4,)), dma((2, 9)), *Exchange.scratch(d)],
        compiler_params=pltpu.CompilerParams(collective_id=0, has_side_effects=True, vmem_limit_bytes=VMEM_LIMIT),
        name='forward',
    )(x, mask, vec, bup, wqkv, wout, wup, wdown)


def run_backward(dy, vec, wqkv, wout, wup, wdown, x_s, hid_s, qkv_s, p_s, u_s):
    n, d = wqkv.shape[0], dy.shape[-1]
    shape = jax.ShapeDtypeStruct
    dma = pltpu.SemaphoreType.DMA
    outs = [shape((4, 32, d), F32), shape((n, 4, 128, d), BF), shape((n, 4, 128, d), BF), shape((n, 4, 128, d), BF),
            shape((n, 4, 128, 1536), BF), shape((n, d), F32), shape((6, n, d), F32)]
    return pl.pallas_call(
        backward_kernel,
        in_specs=[vmem_spec()] * 2 + [any_spec()] * 9,
        out_specs=[vmem_spec()] + [any_spec()] * 4 + [vmem_spec()] * 2,
        out_shape=outs,
        scratch_shapes=[pltpu.VMEM((1536, d), BF), pltpu.VMEM((512, d), BF), pltpu.VMEM((d, d), BF), pltpu.VMEM((d, d), BF)]
                       + [pltpu.VMEM((4, 32, d), F32)] * 4
                       + [pltpu.VMEM((4, 128, d), BF), pltpu.VMEM((4, 128, d), BF), pltpu.VMEM((4, 128, 1536), BF), pltpu.VMEM((4, 4, 256, 128), F32),
                          pltpu.VMEM((4, 128, d), F32), pltpu.VMEM((4, 128, d), BF), pltpu.VMEM((4, 128, 512), BF), pltpu.VMEM((4, 128, 1536), BF),
                          pltpu.VMEM((6, n, d), F32), pltpu.VMEM((2, 6, n, d), F32),
                          dma((4,)), dma((5,)), dma((2, 4)), dma((2, 2)), *Exchange.scratch(d)],
        compiler_params=pltpu.CompilerParams(collective_id=1, has_side_effects=True, vmem_limit_bytes=VMEM_LIMIT),
        name='backward',
    )(dy, vec, wqkv, wout, wup, wdown, x_s, hid_s, qkv_s, p_s, u_s)


def wgrad_kernel(a, b, out):
    out[0] = dot_tn(a[0], b[0]).astype(BF)


def weight_grad(a, b):
    n, rows, m = a.shape
    width = b.shape[2]
    tm = 256
    return pl.pallas_call(
        wgrad_kernel,
        grid=(n, m // tm),
        in_specs=[pl.BlockSpec((1, rows, tm), lambda l, i: (l, 0, i)), pl.BlockSpec((1, rows, width), lambda l, i: (l, 0, 0))],
        out_specs=pl.BlockSpec((1, tm, width), lambda l, i: (l, i, 0)),
        out_shape=jax.ShapeDtypeStruct((n, m, width), BF),
        compiler_params=pltpu.CompilerParams(vmem_limit_bytes=32 * 1024 * 1024),
        cost_estimate=pl.CostEstimate(flops=2 * n * rows * m * width, bytes_accessed=2 * n * (m * width + rows * (m + width)), transcendentals=0),
        name='weight_grad',
    )(a, b)


def group_body(x_loc, dy_loc, len_loc, wqkv_loc, wout_loc, wup_loc, bup_loc, wdown_loc, vec_loc):
    n, d = wqkv_loc.shape[0], x_loc.shape[-1]
    me = lax.axis_index(TENSOR_AXIS)
    row = jnp.arange(128, dtype=jnp.int32)
    pos = ((row // 32) ^ me) * 32 + row % 32
    visible = (pos[None, None, :] <= pos[None, :, None]) & (pos[None, None, :] < len_loc[:, None, None])
    mask = visible.astype(F32)
    vec = vec_loc.transpose(1, 0, 2)
    wqkv = wqkv_loc.transpose(0, 2, 3, 4, 1).reshape(n, 1536, d)
    wout = wout_loc.reshape(n, 512, d)
    y, x_s, hid_s, a_s, qkv_s, ctx_s, p_s, m_s, u_s, act_s = run_forward(x_loc, mask, vec, bup_loc, wqkv, wout, wup_loc, wdown_loc)
    d_x, dmlp_s, dpre_s, dattn_s, dqkv_s, g_bup, g_vec = run_backward(dy_loc, vec, wqkv, wout, wup_loc, wdown_loc, x_s, hid_s, qkv_s, p_s, u_s)

    def tokens(val):
        return val.reshape(n, 512, val.shape[-1])

    g_qkv = weight_grad(tokens(dqkv_s), tokens(a_s)).reshape(n, 3, 8, 64, d).transpose(0, 4, 1, 2, 3)
    g_out = weight_grad(tokens(ctx_s), tokens(dattn_s)).reshape(n, 8, 64, d)
    g_up = weight_grad(tokens(m_s), tokens(dpre_s))
    g_down = weight_grad(tokens(act_s), tokens(dmlp_s))
    return y, d_x, g_qkv, g_out, g_up, g_bup, g_down, g_vec.transpose(1, 0, 2)


def solution(mesh):
    act_spec = P(PARTS_AXIS, TENSOR_AXIS, None)
    in_specs = (act_spec, act_spec, P(PARTS_AXIS), P(None, None, None, TENSOR_AXIS, None), P(None, TENSOR_AXIS, None, None), P(None, None, TENSOR_AXIS), P(None, TENSOR_AXIS), P(None, TENSOR_AXIS, None), P())
    out_specs = (act_spec, act_spec, P(PARTS_AXIS, None, None, TENSOR_AXIS, None), P(PARTS_AXIS, TENSOR_AXIS, None, None), P(PARTS_AXIS, None, TENSOR_AXIS), P(PARTS_AXIS, TENSOR_AXIS), P(PARTS_AXIS, TENSOR_AXIS, None), P(PARTS_AXIS, None, None))
    return jax.shard_map(group_body, mesh=mesh, in_specs=in_specs, out_specs=out_specs, check_vma=False)
```

```python
import functools
import jax
import jax.numpy as jnp
from jax import lax
from jax.experimental import pallas as pl
from jax.experimental.pallas import tpu as pltpu
from jax.sharding import PartitionSpec as P

TENSOR_AXIS = 'tp'
PARTS_AXIS = 'dp'
BF = jnp.bfloat16
F32 = jnp.float32
MESH = pl.DeviceIdType.MESH
VMEM_LIMIT = 67043328
NUM_CHUNKS = 2
RS_BLOCKS = 2
GELU_C = 0.7978845608028654


def dot_nn(a, b):
    return lax.dot_general(a, b, (((1,), (0,)), ((), ())), preferred_element_type=F32)


def dot_nt(a, b):
    return lax.dot_general(a, b, (((1,), (1,)), ((), ())), preferred_element_type=F32)


def dot_tn(a, b):
    return lax.dot_general(a, b, (((0,), (0,)), ((), ())), preferred_element_type=F32)


def seqs(c):
    return pl.ds(2 * c, 2)


def rows_of(ref, c):
    val = ref[seqs(c)]
    return val.reshape(256, val.shape[-1])


def normed(z):
    mean = jnp.mean(z, axis=-1, keepdims=True)
    centered = z - mean
    var = jnp.mean(centered * centered, axis=-1, keepdims=True)
    rstd = lax.rsqrt(var + 1e-5)
    return centered * rstd, rstd


class Exchange:
    def __init__(self, part, from_core, far_send, far_recv, sems):
        self.me = lax.axis_index(TENSOR_AXIS)
        self.part, self.from_core = part, from_core
        self.far_send, self.far_recv = far_send, far_recv
        self.gs, self.gr, self.cs, self.cr, self.xs, self.xr = sems

    def remote(self, src, dst, send, recv, flip):
        return pltpu.make_async_remote_copy(
            src_ref=src, dst_ref=dst, send_sem=send, recv_sem=recv,
            device_id={TENSOR_AXIS: lax.bitwise_xor(self.me, flip)}, device_id_type=MESH)

    def barrier(self):
        sem = pltpu.get_barrier_semaphore()
        for flip in (1, 2):
            pl.semaphore_signal(sem, inc=1, device_id={TENSOR_AXIS: lax.bitwise_xor(self.me, flip)}, device_id_type=MESH)
        pl.semaphore_wait(sem, 2)

    def gather(self, buf, c):
        return self.remote(buf.at[seqs(c), pl.ds(0, 64)], buf.at[seqs(c), pl.ds(64, 64)], self.gs.at[c], self.gr.at[c], 1)

    def cols(self, b):
        width = self.part.shape[-1] // RS_BLOCKS
        return pl.ds(b * width, width)

    def core_copy(self, c, b):
        return self.remote(self.part.at[seqs(c), pl.ds(64, 64), self.cols(b)], self.from_core.at[seqs(c), :, self.cols(b)],
                           self.cs.at[c, b], self.cr.at[c, b], 1)

    def far_copy(self, kind, c, b, full):
        rows = pl.ds(0, 64) if full else pl.ds(32, 32)
        return self.remote(self.far_send.at[seqs(c), rows, self.cols(b)], self.far_recv.at[kind, seqs(c), rows, self.cols(b)],
                           self.xs.at[kind, c, b], self.xr.at[kind, c, b], 2)

    def middle(self, kind, c, full):
        for b in range(RS_BLOCKS):
            self.core_copy(c, b).wait_recv()
            near = self.part[seqs(c), pl.ds(0, 64), self.cols(b)].astype(F32)
            self.far_send[seqs(c), :, self.cols(b)] = (near + self.from_core[seqs(c), :, self.cols(b)].astype(F32)).astype(BF)
            if full is True:
                self.far_copy(kind, c, b, True).start()
            else:
                @pl.when(full)
                def _():
                    self.far_copy(kind, c, b, True).start()

                @pl.when(jnp.logical_not(full))
                def _():
                    self.far_copy(kind, c, b, False).start()

    def finish(self, kind, c, full):
        for b in range(RS_BLOCKS):
            self.far_copy(kind, c, b, full).wait_recv()
            self.far_copy(kind, c, b, full).wait_send()
            self.core_copy(c, b).wait_send()
        own = self.far_send[seqs(c), pl.ds(0, 32)].astype(F32) + self.far_recv[kind, seqs(c), pl.ds(32, 32)].astype(F32)
        own = own.astype(BF).astype(F32)
        if not full:
            return own
        twin = self.far_send[seqs(c), pl.ds(32, 32)].astype(F32) + self.far_recv[kind, seqs(c), pl.ds(0, 32)].astype(F32)
        return jnp.concatenate([own, twin.astype(BF).astype(F32)], axis=1)

    @staticmethod
    def scratch(d):
        dma = pltpu.SemaphoreType.DMA
        return [pltpu.VMEM((4, 128, d), BF), pltpu.VMEM((4, 64, d), BF), pltpu.VMEM((4, 64, d), BF), pltpu.VMEM((2, 4, 64, d), BF),
                dma((2,)), dma((2,)), dma((2, RS_BLOCKS)), dma((2, RS_BLOCKS)), dma((2, 2, RS_BLOCKS)), dma((2, 2, RS_BLOCKS))]


def partial_sum(ex, c, block_of, bn=512):
    width = ex.part.shape[-1] // RS_BLOCKS
    for b in range(RS_BLOCKS):
        @pl.loop(0, width // bn)
        def _(j):
            cols = pl.ds(pl.multiple_of(b * width + j * bn, bn), bn)
            ex.part[seqs(c), :, cols] = block_of(cols).astype(BF).reshape(2, 128, bn)

        ex.core_copy(c, b).start()


def lane_low():
    return lax.broadcasted_iota(jnp.int32, (128, 128), 1) < 64


def two_heads(val, low):
    zero = jnp.zeros_like(val)
    return jnp.concatenate([jnp.where(low, val, zero), jnp.where(low, zero, val)], axis=0)


def forward_kernel(x_in, mask, vec, bup, wqkv_h, wout_h, wup_h, wdown_h,
                   y_out, x_s, hid_s, a_s, qkv_s, ctx_s, p_s, m_s, u_s, act_s,
                   wq, wo, wu, wd, xbuf, hbuf, ag_a, ag_m, qkv, ctx, prob, u, act,
                   wsem, ssem, isem, part, from_core, far_send, far_recv, *sems):
    n_layers = wqkv_h.shape[0]
    ex = Exchange(part, from_core, far_send, far_recv, sems)

    def weight_copies(l, kind):
        pairs = ((wqkv_h, wq, 0), (wout_h, wo, 1)) if kind == 0 else ((wup_h, wu, 2), (wdown_h, wd, 3))
        return [pltpu.make_async_copy(src.at[l], dst, wsem.at[i]) for src, dst, i in pairs]

    def save_copies(l, c, kind):
        if kind == 0:
            pairs = ((xbuf, x_s, 0), (ag_a, a_s, 1), (qkv, qkv_s, 2), (ctx, ctx_s, 3), (prob, p_s, 4))
        else:
            pairs = ((hbuf, hid_s, 5), (ag_m, m_s, 6), (u, u_s, 7), (act, act_s, 8))
        return [pltpu.make_async_copy(src.at[seqs(c)], dst.at[l, seqs(c)], ssem.at[c, i]) for src, dst, i in pairs]

    def norm_and_gather(src, l, c, row, buf):
        xhat, _ = normed(src[seqs(c)].reshape(128, -1))
        val = xhat * vec[row, pl.ds(l, 1), :] + vec[row + 1, pl.ds(l, 1), :]
        buf[seqs(c), pl.ds(0, 64)] = val.astype(BF).reshape(2, 64, -1)
        ex.gather(buf, c).start()
        ex.gather(buf, c).wait()

    def first_copy(c):
        return ex.remote(x_in.at[seqs(c)], xbuf.at[seqs(c), pl.ds(32, 32)], isem.at[0, c], isem.at[1, c], 2)

    def attention(c):
        a = rows_of(ag_a, c)
        for j in range(3):
            cols = pl.ds(512 * j, 512)
            qkv[seqs(c), :, cols] = dot_nt(a, wq[cols, :]).astype(BF).reshape(2, 128, 512)
        low = lane_low()

        @pl.loop(0, 2)
        def _(s):
            seq = 2 * c + s
            visible = mask[seq] > 0
            visible = jnp.concatenate([visible, visible], axis=0)
            for pair in range(4):
                q, k, v = (qkv[seq, :, pl.ds(512 * t + 128 * pair, 128)] for t in range(3))
                scores = dot_nt(two_heads(q, low), k) * 0.125
                scores = jnp.where(visible, scores, -1e30)
                e = jnp.exp(scores - jnp.max(scores, axis=-1, keepdims=True))
                p = e / jnp.sum(e, axis=-1, keepdims=True)
                prob[seq, pair] = p
                pb = p.astype(BF)
                both = jnp.concatenate([pb[:128], pb[128:]], axis=1)
                ctx[seq, :, pl.ds(128 * pair, 128)] = dot_nn(both, two_heads(v, low)).astype(BF)

    def mlp(l, c):
        m = rows_of(ag_m, c)

        @pl.loop(0, 4)
        def _(j):
            cols = pl.ds(pl.multiple_of(512 * j, 512), 512)
            pre = dot_nn(m, wu[:, cols]) + bup[pl.ds(l, 1), cols]
            u[seqs(c), :, cols] = pre.reshape(2, 128, 512)
            t = jnp.tanh(GELU_C * (pre + 0.044715 * (pre * pre * pre)))
            act[seqs(c), :, cols] = (0.5 * pre * (1.0 + t)).astype(BF).reshape(2, 128, 512)

    for kind in range(2):
        for copy in weight_copies(0, kind):
            copy.start()
    ex.barrier()
    for c in range(NUM_CHUNKS):
        first_copy(c).start()
    xbuf[:, pl.ds(0, 32)] = x_in[...]

    @pl.loop(0, n_layers)
    def _(l):
        for c in range(NUM_CHUNKS):
            @pl.when(l == 0)
            def _():
                first_copy(c).wait()

            @pl.when(l > 0)
            def _():
                xbuf[seqs(c)] = hbuf[seqs(c)] + ex.finish(1, c, True) + vec[5, pl.ds(l - 1, 1), :][None]

            norm_and_gather(xbuf, l, c, 0, ag_a)
            if c == 0:
                for copy in weight_copies(l, 0):
                    copy.wait()
            attention(c)
            for copy in save_copies(l, c, 0):
                copy.start()
            lhs = rows_of(ctx, c)
            partial_sum(ex, c, lambda cols: dot_nn(lhs, wo[:, cols]))
            ex.middle(0, c, True)

        @pl.when(l + 1 < n_layers)
        def _():
            for copy in weight_copies(l + 1, 0):
                copy.start()

        for c in range(NUM_CHUNKS):
            hbuf[seqs(c)] = xbuf[seqs(c)] + ex.finish(0, c, True) + vec[4, pl.ds(l, 1), :][None]
            norm_and_gather(hbuf, l, c, 2, ag_m)
            if c == 0:
                for copy in weight_copies(l, 1):
                    copy.wait()
            mlp(l, c)
            for copy in save_copies(l, c, 1):
                copy.start()
            for copy in save_copies(l, c, 0):
                copy.wait()
            lhs = rows_of(act, c)
            partial_sum(ex, c, lambda cols: dot_nn(lhs, wd[:, cols]))
            ex.middle(1, c, l + 1 < n_layers)

        @pl.when(l + 1 < n_layers)
        def _():
            for copy in weight_copies(l + 1, 1):
                copy.start()

        for c in range(NUM_CHUNKS):
            for copy in save_copies(l, c, 1):
                copy.wait()

    for c in range(NUM_CHUNKS):
        y_out[seqs(c)] = hbuf[seqs(c), pl.ds(0, 32)] + ex.finish(1, c, False) + vec[5, pl.ds(n_layers - 1, 1), :][None]


def backward_kernel(dy_in, vec, wqkv_h, wout_h, wup_h, wdown_h, x_s, hid_s, qkv_s, p_s, u_s,
                    d_x, dmlp_s, dpre_s, dattn_s, dqkv_s, g_bup, g_vec,
                    wq, wo, wu, wd, dcur, dhid, zbuf, ag_a, ag_m, qkv, prob, u, dpre, dctx, dqkv, vacc, vfar, vlast,
                    wsem, rsem, zsem, ssem, vsem, isem, part, from_core, far_send, far_recv, *sems):
    n_layers = wqkv_h.shape[0]
    ex = Exchange(part, from_core, far_send, far_recv, sems)

    def loads(l, kind):
        if kind == 0:
            whole = ((wqkv_h, wq, 0), (wout_h, wo, 1))
            saved = ((qkv_s, qkv, 1), (p_s, prob, 2))
        else:
            whole = ((wdown_h, wd, 3), (wup_h, wu, 2))
            saved = ((u_s, u, 0),)
        return ([pltpu.make_async_copy(src.at[l], dst, wsem.at[i]) for src, dst, i in whole]
                + [pltpu.make_async_copy(src.at[l], dst, rsem.at[i]) for src, dst, i in saved])

    def z_load(l, c, kind):
        return pltpu.make_async_copy((x_s, hid_s)[kind].at[l, seqs(c)], zbuf.at[seqs(c)], zsem.at[c])

    def save_copies(l, c, kind):
        pairs = ((ag_a, dattn_s, 0), (dqkv, dqkv_s, 1)) if kind == 0 else ((ag_m, dmlp_s, 2), (dpre, dpre_s, 3))
        return [pltpu.make_async_copy(src.at[seqs(c)], dst.at[l, seqs(c)], ssem.at[c, i]) for src, dst, i in pairs]

    def send(src, c, buf):
        buf[seqs(c), pl.ds(0, 64)] = src[seqs(c)].astype(BF)
        ex.gather(buf, c).start()
        ex.gather(buf, c).wait()

    def first_copy(c):
        return ex.remote(dy_in.at[seqs(c)], far_recv.at[0, seqs(c), pl.ds(0, 32)], isem.at[0, c], isem.at[1, c], 2)

    def dx_copy(c):
        return pltpu.make_async_copy(dcur.at[seqs(c), pl.ds(0, 32)], d_x.at[seqs(c)], isem.at[0, c])

    def row_sum(val):
        sums = [jnp.sum(val[:, 32 * i:32 * i + 32].reshape(64, -1), axis=0, keepdims=True) for i in range(val.shape[1] // 32)]
        return sums[0] if len(sums) == 1 else sums[0] + sums[1]

    def add_row(i, l, c, val):
        row = (i, pl.ds(l, 1))
        total = row_sum(val)
        vacc[row] = total if c == 0 else vacc[row] + total

    def norm_bwd(z, d_z, gain):
        shape = z.shape
        z, d_z = z.reshape(-1, shape[-1]), d_z.reshape(-1, shape[-1])
        xhat, rstd = normed(z)
        g = d_z * gain
        g_mean = jnp.mean(g, axis=-1, keepdims=True)
        gx_mean = jnp.mean(g * xhat, axis=-1, keepdims=True)
        return (rstd * (g - g_mean - xhat * gx_mean)).reshape(shape), (d_z * xhat).reshape(shape)

    def mlp_bwd(l, c):
        d_mlp = rows_of(ag_m, c)

        @pl.loop(0, 4)
        def _(j):
            cols = pl.ds(pl.multiple_of(512 * j, 512), 512)
            d_act = dot_nt(d_mlp, wd[cols, :]).astype(BF).astype(F32)
            pre = u[seqs(c), :, cols].reshape(256, 512)
            sq = pre * pre
            t = jnp.tanh(GELU_C * (pre + 0.044715 * (sq * pre)))
            slope = 0.5 * (1.0 + t) + 0.5 * pre * (1.0 - t * t) * (GELU_C * (1.0 + 0.134145 * sq))
            d_pre = d_act * slope
            total = jnp.sum(d_pre, axis=0, keepdims=True)
            g_bup[pl.ds(l, 1), cols] = total if c == 0 else g_bup[pl.ds(l, 1), cols] + total
            dpre[seqs(c), :, cols] = d_pre.astype(BF).reshape(2, 128, 512)

    def attention_bwd(c):
        dctx[seqs(c)] = dot_nt(rows_of(ag_a, c), wo[...]).astype(BF).reshape(2, 128, 512)
        low = lane_low()

        @pl.loop(0, 2)
        def _(s):
            seq = 2 * c + s
            for pair in range(4):
                q, k, v = (qkv[seq, :, pl.ds(512 * t + 128 * pair, 128)] for t in range(3))
                d_c = two_heads(dctx[seq, :, pl.ds(128 * pair, 128)], low)
                p = prob[seq, pair]
                d_p = dot_nt(d_c, v).astype(BF).astype(F32)
                d_s = p * (d_p - jnp.sum(d_p * p, axis=-1, keepdims=True))
                d_s = (d_s * 0.125).astype(BF)
                both = jnp.concatenate([d_s[:128], d_s[128:]], axis=1)
                d_q = dot_nn(both, two_heads(k, low))
                d_k = dot_tn(d_s, two_heads(q, low))
                d_v = dot_tn(p.astype(BF), d_c)
                for t, val in enumerate((d_q, d_k, d_v)):
                    dqkv[seq, :, pl.ds(512 * t + 128 * pair, 128)] = val.astype(BF)

    last = n_layers - 1
    for kind in (1, 0):
        for copy in loads(last, kind):
            copy.start()
    for c in range(NUM_CHUNKS):
        z_load(last, c, 1).start()
    ex.barrier()
    for c in range(NUM_CHUNKS):
        first_copy(c).start()
    dcur[:, pl.ds(0, 32)] = dy_in[...].astype(F32)

    @pl.loop(0, n_layers)
    def _(i):
        l = last - i

        for c in range(NUM_CHUNKS):
            @pl.when(i == 0)
            def _():
                first_copy(c).wait()
                dcur[seqs(c), pl.ds(32, 32)] = far_recv[0, seqs(c), pl.ds(0, 32)].astype(F32)

            @pl.when(i > 0)
            def _():
                d_in = ex.finish(0, c, True)
                z_load(l + 1, c, 0).wait()
                d_ln, d_gain = norm_bwd(zbuf[seqs(c)], d_in, vec[0, pl.ds(l + 1, 1), :])
                z_load(l, c, 1).start()
                dcur[seqs(c)] = dhid[seqs(c)] + d_ln
                add_row(0, l + 1, c, d_gain)
                add_row(1, l + 1, c, d_in)

            send(dcur, c, ag_m)
            add_row(5, l, c, dcur[seqs(c)])
            if c == 0:
                for copy in loads(l, 1):
                    copy.wait()
            mlp_bwd(l, c)
            for copy in save_copies(l, c, 1):
                copy.start()

            @pl.when(i > 0)
            def _():
                for copy in save_copies(l + 1, c, 0):
                    copy.wait()

            lhs = rows_of(dpre, c)
            partial_sum(ex, c, lambda cols: dot_nt(lhs, wu[cols, :]))
            ex.middle(1, c, True)

        for c in range(NUM_CHUNKS):
            d_mid = ex.finish(1, c, True)
            z_load(l, c, 1).wait()
            d_ln, d_gain = norm_bwd(zbuf[seqs(c)], d_mid, vec[2, pl.ds(l, 1), :])
            z_load(l, c, 0).start()
            dhid[seqs(c)] = dcur[seqs(c)] + d_ln
            send(dhid, c, ag_a)
            add_row(2, l, c, d_gain)
            add_row(3, l, c, d_mid)
            add_row(4, l, c, dhid[seqs(c)])
            if c == 0:
                for copy in loads(l, 0):
                    copy.wait()
            else:
                @pl.when(l > 0)
                def _():
                    for copy in loads(l - 1, 1):
                        copy.start()

            attention_bwd(c)
            for copy in save_copies(l, c, 0):
                copy.start()
            for copy in save_copies(l, c, 1):
                copy.wait()
            lhs = rows_of(dqkv, c)
            partial_sum(ex, c, lambda cols: dot_nn(lhs, wq[:, cols]))
            ex.middle(0, c, l > 0)

        @pl.when(l > 0)
        def _():
            for copy in loads(l - 1, 0):
                copy.start()

    for c in range(NUM_CHUNKS):
        z_load(0, c, 0).wait()
        for copy in save_copies(0, c, 0):
            copy.wait()
        d_in = ex.finish(0, c, False)
        d_ln, d_gain = norm_bwd(zbuf[seqs(c), pl.ds(0, 32)], d_in, vec[0, pl.ds(0, 1), :])
        dcur[seqs(c), pl.ds(0, 32)] = dhid[seqs(c), pl.ds(0, 32)] + d_ln
        dx_copy(c).start()
        for row, val in enumerate((d_gain, d_in)):
            total = row_sum(val)
            at = (0, pl.ds(row, 1))
            vlast[at] = total if c == 0 else vlast[at] + total
    copy = ex.remote(vlast.at[0], vlast.at[1], vsem.at[0, 0], vsem.at[0, 1], 2)
    copy.start()
    copy.wait()
    for row in range(2):
        vacc[row, pl.ds(0, 1)] = vlast[0, pl.ds(row, 1)] + vlast[1, pl.ds(row, 1)]
    copy = ex.remote(vacc, vfar, vsem.at[1, 0], vsem.at[1, 1], 1)
    copy.start()
    copy.wait()
    g_vec[...] = vacc[...] + vfar[...]
    for c in range(NUM_CHUNKS):
        dx_copy(c).wait()


def any_spec():
    return pl.BlockSpec(memory_space=pl.ANY)


def vmem_spec():
    return pl.BlockSpec(memory_space=pltpu.VMEM)


def run_forward(x, mask, vec, bup, wqkv, wout, wup, wdown):
    n, d = wqkv.shape[0], x.shape[-1]
    shape = jax.ShapeDtypeStruct
    dma = pltpu.SemaphoreType.DMA
    outs = [shape((4, 32, d), F32), shape((n, 4, 64, d), F32), shape((n, 4, 64, d), F32), shape((n, 4, 128, d), BF),
            shape((n, 4, 128, 1536), BF), shape((n, 4, 128, 512), BF), shape((n, 4, 4, 256, 128), F32),
            shape((n, 4, 128, d), BF), shape((n, 4, 128, d), F32), shape((n, 4, 128, d), BF)]
    return pl.pallas_call(
        forward_kernel,
        in_specs=[vmem_spec()] * 4 + [any_spec()] * 4,
        out_specs=[vmem_spec()] + [any_spec()] * 9,
        out_shape=outs,
        scratch_shapes=[pltpu.VMEM((1536, d), BF), pltpu.VMEM((512, d), BF), pltpu.VMEM((d, d), BF), pltpu.VMEM((d, d), BF),
                        pltpu.VMEM((4, 64, d), F32), pltpu.VMEM((4, 64, d), F32), pltpu.VMEM((4, 128, d), BF), pltpu.VMEM((4, 128, d), BF),
                        pltpu.VMEM((4, 128, 1536), BF), pltpu.VMEM((4, 128, 512), BF), pltpu.VMEM((4, 4, 256, 128), F32),
                        pltpu.VMEM((4, 128, d), F32), pltpu.VMEM((4, 128, d), BF), dma((4,)), dma((2, 9)), dma((2, 2)), *Exchange.scratch(d)],
        compiler_params=pltpu.CompilerParams(collective_id=0, has_side_effects=True, vmem_limit_bytes=VMEM_LIMIT),
        name='forward',
    )(x, mask, vec, bup, wqkv, wout, wup, wdown)


def run_backward(dy, vec, wqkv, wout, wup, wdown, x_s, hid_s, qkv_s, p_s, u_s):
    n, d = wqkv.shape[0], dy.shape[-1]
    shape = jax.ShapeDtypeStruct
    dma = pltpu.SemaphoreType.DMA
    outs = [shape((4, 32, d), F32), shape((n, 4, 128, d), BF), shape((n, 4, 128, d), BF), shape((n, 4, 128, d), BF),
            shape((n, 4, 128, 1536), BF), shape((n, d), F32), shape((6, n, d), F32)]
    return pl.pallas_call(
        backward_kernel,
        in_specs=[vmem_spec()] * 2 + [any_spec()] * 9,
        out_specs=[any_spec()] * 5 + [vmem_spec()] * 2,
        out_shape=outs,
        scratch_shapes=[pltpu.VMEM((1536, d), BF), pltpu.VMEM((512, d), BF), pltpu.VMEM((d, d), BF), pltpu.VMEM((d, d), BF)]
                       + [pltpu.VMEM((4, 64, d), F32)] * 3
                       + [pltpu.VMEM((4, 128, d), BF), pltpu.VMEM((4, 128, d), BF), pltpu.VMEM((4, 128, 1536), BF), pltpu.VMEM((4, 4, 256, 128), F32),
                          pltpu.VMEM((4, 128, d), F32), pltpu.VMEM((4, 128, d), BF), pltpu.VMEM((4, 128, 512), BF), pltpu.VMEM((4, 128, 1536), BF),
                          pltpu.VMEM((6, n, d), F32), pltpu.VMEM((6, n, d), F32), pltpu.VMEM((2, 2, d), F32),
                          dma((4,)), dma((3,)), dma((2,)), dma((2, 4)), dma((2, 2)), dma((2, 2)), *Exchange.scratch(d)],
        compiler_params=pltpu.CompilerParams(collective_id=1, has_side_effects=True, vmem_limit_bytes=VMEM_LIMIT),
        name='backward',
    )(dy, vec, wqkv, wout, wup, wdown, x_s, hid_s, qkv_s, p_s, u_s)


def wgrad_kernel(a, b, out):
    out[0] = dot_tn(a[0], b[0]).astype(BF)


def weight_grad(a, b):
    n, rows, m = a.shape
    width = b.shape[2]
    tm = {2048: 1024, 1536: 768, 512: 512}[m]
    return pl.pallas_call(
        wgrad_kernel,
        grid=(n, m // tm),
        in_specs=[pl.BlockSpec((1, rows, tm), lambda l, i: (l, 0, i)), pl.BlockSpec((1, rows, width), lambda l, i: (l, 0, 0))],
        out_specs=pl.BlockSpec((1, tm, width), lambda l, i: (l, i, 0)),
        out_shape=jax.ShapeDtypeStruct((n, m, width), BF),
        compiler_params=pltpu.CompilerParams(vmem_limit_bytes=VMEM_LIMIT),
        cost_estimate=pl.CostEstimate(flops=2 * n * rows * m * width, bytes_accessed=2 * n * (m * width + rows * (m + width)), transcendentals=0),
        name='weight_grad',
    )(a, b)


def group_body(x_loc, dy_loc, len_loc, wqkv_loc, wout_loc, wup_loc, bup_loc, wdown_loc, vec_loc):
    n, d = wqkv_loc.shape[0], x_loc.shape[-1]
    me = lax.axis_index(TENSOR_AXIS)
    row = jnp.arange(128, dtype=jnp.int32)
    block = (row // 32) // 2 + 2 * ((row // 32) % 2)
    pos = (block ^ me) * 32 + row % 32
    visible = (pos[None, None, :] <= pos[None, :, None]) & (pos[None, None, :] < len_loc[:, None, None])
    mask = visible.astype(F32)
    vec = vec_loc.transpose(1, 0, 2)
    wqkv = wqkv_loc.transpose(0, 2, 3, 4, 1).reshape(n, 1536, d)
    wout = wout_loc.reshape(n, 512, d)
    y, x_s, hid_s, a_s, qkv_s, ctx_s, p_s, m_s, u_s, act_s = run_forward(x_loc, mask, vec, bup_loc, wqkv, wout, wup_loc, wdown_loc)
    d_x, dmlp_s, dpre_s, dattn_s, dqkv_s, g_bup, g_vec = run_backward(dy_loc, vec, wqkv, wout, wup_loc, wdown_loc, x_s, hid_s, qkv_s, p_s, u_s)

    def tokens(val):
        return val.reshape(n, 512, val.shape[-1])

    g_qkv = weight_grad(tokens(dqkv_s), tokens(a_s)).reshape(n, 3, 8, 64, d).transpose(0, 4, 1, 2, 3)
    g_out = weight_grad(tokens(ctx_s), tokens(dattn_s)).reshape(n, 8, 64, d)
    g_up = weight_grad(tokens(m_s), tokens(dpre_s))
    g_down = weight_grad(tokens(act_s), tokens(dmlp_s))
    return y, d_x, g_qkv, g_out, g_up, g_bup, g_down, g_vec.transpose(1, 0, 2)


def solution(mesh):
    act_spec = P(PARTS_AXIS, TENSOR_AXIS, None)
    in_specs = (act_spec, act_spec, P(PARTS_AXIS), P(None, None, None, TENSOR_AXIS, None), P(None, TENSOR_AXIS, None, None), P(None, None, TENSOR_AXIS), P(None, TENSOR_AXIS), P(None, TENSOR_AXIS, None), P())
    out_specs = (act_spec, act_spec, P(PARTS_AXIS, None, None, TENSOR_AXIS, None), P(PARTS_AXIS, TENSOR_AXIS, None, None), P(PARTS_AXIS, None, TENSOR_AXIS), P(PARTS_AXIS, TENSOR_AXIS), P(PARTS_AXIS, TENSOR_AXIS, None), P(PARTS_AXIS, None, None))
    return jax.shard_map(group_body, mesh=mesh, in_specs=in_specs, out_specs=out_specs, check_vma=False)
```

```python
import functools
import jax
import jax.numpy as jnp
from jax import lax
from jax.experimental import pallas as pl
from jax.experimental.pallas import tpu as pltpu
from jax.sharding import PartitionSpec as P

TENSOR_AXIS = 'tp'
PARTS_AXIS = 'dp'
BF = jnp.bfloat16
F32 = jnp.float32
MESH = pl.DeviceIdType.MESH
VMEM_LIMIT = 67043328
NUM_CHUNKS = 2
RS_BLOCKS = 4
GELU_C = 0.7978845608028654


def dot_nn(a, b):
    return lax.dot_general(a, b, (((1,), (0,)), ((), ())), preferred_element_type=F32)


def dot_nt(a, b):
    return lax.dot_general(a, b, (((1,), (1,)), ((), ())), preferred_element_type=F32)


def dot_tn(a, b):
    return lax.dot_general(a, b, (((0,), (0,)), ((), ())), preferred_element_type=F32)


def seqs(c):
    return pl.ds(2 * c, 2)


def rows_of(ref, c):
    val = ref[seqs(c)]
    return val.reshape(256, val.shape[-1])


def normed(z):
    mean = jnp.mean(z, axis=-1, keepdims=True)
    centered = z - mean
    var = jnp.mean(centered * centered, axis=-1, keepdims=True)
    rstd = lax.rsqrt(var + 1e-5)
    return centered * rstd, rstd


class Exchange:
    def __init__(self, part, from_core, far_send, far_recv, sems):
        self.me = lax.axis_index(TENSOR_AXIS)
        self.part, self.from_core = part, from_core
        self.far_send, self.far_recv = far_send, far_recv
        self.gs, self.gr, self.cs, self.cr, self.xs, self.xr = sems

    def remote(self, src, dst, send, recv, flip):
        return pltpu.make_async_remote_copy(
            src_ref=src, dst_ref=dst, send_sem=send, recv_sem=recv,
            device_id={TENSOR_AXIS: lax.bitwise_xor(self.me, flip)}, device_id_type=MESH)

    def barrier(self):
        sem = pltpu.get_barrier_semaphore()
        for flip in (1, 2):
            pl.semaphore_signal(sem, inc=1, device_id={TENSOR_AXIS: lax.bitwise_xor(self.me, flip)}, device_id_type=MESH)
        pl.semaphore_wait(sem, 2)

    def gather(self, buf, seq):
        return self.remote(buf.at[seq, pl.ds(0, 64)], buf.at[seq, pl.ds(64, 64)], self.gs.at[seq], self.gr.at[seq], 1)

    def gather_wait(self, buf, c):
        for s in range(2):
            self.gather(buf, 2 * c + s).wait()

    def cols(self, b):
        width = self.part.shape[-1] // RS_BLOCKS
        return pl.ds(pl.multiple_of(b * width, width), width)

    def core_copy(self, c, b):
        return self.remote(self.part.at[seqs(c), pl.ds(64, 64), self.cols(b)], self.from_core.at[seqs(c), :, self.cols(b)],
                           self.cs.at[c, b], self.cr.at[c, b], 1)

    def far_copy(self, kind, c, b, full):
        rows = pl.ds(0, 64) if full else pl.ds(32, 32)
        return self.remote(self.far_send.at[seqs(c), rows, self.cols(b)], self.far_recv.at[kind, seqs(c), rows, self.cols(b)],
                           self.xs.at[kind, c, b], self.xr.at[kind, c, b], 2)

    def middle(self, kind, c, b, full):
        self.core_copy(c, b).wait_recv()
        near = self.part[seqs(c), pl.ds(0, 64), self.cols(b)].astype(F32)
        self.far_send[seqs(c), :, self.cols(b)] = (near + self.from_core[seqs(c), :, self.cols(b)].astype(F32)).astype(BF)
        if isinstance(full, bool):
            self.far_copy(kind, c, b, full).start()
        else:
            @pl.when(full)
            def _():
                self.far_copy(kind, c, b, True).start()

            @pl.when(jnp.logical_not(full))
            def _():
                self.far_copy(kind, c, b, False).start()

    def finish(self, kind, c, full):
        for b in range(RS_BLOCKS):
            self.far_copy(kind, c, b, full).wait_recv()
            self.far_copy(kind, c, b, full).wait_send()
            self.core_copy(c, b).wait_send()
        own = self.far_send[seqs(c), pl.ds(0, 32)].astype(F32) + self.far_recv[kind, seqs(c), pl.ds(32, 32)].astype(F32)
        own = own.astype(BF).astype(F32)
        if not full:
            return own
        twin = self.far_send[seqs(c), pl.ds(32, 32)].astype(F32) + self.far_recv[kind, seqs(c), pl.ds(0, 32)].astype(F32)
        return jnp.concatenate([own, twin.astype(BF).astype(F32)], axis=1)

    @staticmethod
    def scratch(d):
        dma = pltpu.SemaphoreType.DMA
        return [pltpu.VMEM((4, 128, d), BF), pltpu.VMEM((4, 64, d), BF), pltpu.VMEM((4, 64, d), BF), pltpu.VMEM((2, 4, 64, d), BF),
                dma((4,)), dma((4,)), dma((2, RS_BLOCKS)), dma((2, RS_BLOCKS)), dma((2, 2, RS_BLOCKS)), dma((2, 2, RS_BLOCKS))]


LAST = RS_BLOCKS - 1


def partial_sum(ex, kind, c, full, block_of):
    @pl.loop(0, RS_BLOCKS)
    def _(b):
        cols = ex.cols(b)
        ex.part[seqs(c), :, cols] = block_of(cols).astype(BF).reshape(2, 128, -1)
        ex.core_copy(c, b).start()

        @pl.when(b > 0)
        def _():
            ex.middle(kind, c, b - 1, full)


def lane_low():
    return lax.broadcasted_iota(jnp.int32, (128, 128), 1) < 64


def two_heads(val, low):
    zero = jnp.zeros_like(val)
    return jnp.concatenate([jnp.where(low, val, zero), jnp.where(low, zero, val)], axis=0)


def forward_kernel(x_in, lens, vec, bup, wqkv_h, wout_h, wup_h, wdown_h,
                   y_out, x_s, hid_s, a_s, qkv_s, p_s, slope_s, lhs_s,
                   wq, wo, wu, wd, xbuf, hbuf, ag_a, ag_m, qkv, ctx, prob, slope, act,
                   wsem, ssem, isem, part, from_core, far_send, far_recv, *sems):
    n_layers = wqkv_h.shape[0]
    ex = Exchange(part, from_core, far_send, far_recv, sems)

    d = x_in.shape[-1]

    def lhs_cols(start, width):
        return lhs_s.at[:, :, :, pl.ds(start, width)]

    def weight_copies(l, kind):
        pairs = ((wqkv_h, wq, 0), (wout_h, wo, 1)) if kind == 0 else ((wup_h, wu, 2), (wdown_h, wd, 3))
        return [pltpu.make_async_copy(src.at[l], dst, wsem.at[i]) for src, dst, i in pairs]

    def save_copies(l, c, kind):
        if kind == 0:
            pairs = ((xbuf, x_s, 0), (ag_a, a_s, 1), (qkv, qkv_s, 2), (ctx, lhs_cols(2 * d, 512), 3), (prob, p_s, 4))
        else:
            pairs = ((hbuf, hid_s, 5), (ag_m, lhs_cols(0, d), 6), (slope, slope_s, 7), (act, lhs_cols(d, d), 8))
        return [pltpu.make_async_copy(src.at[seqs(c)], dst.at[l, seqs(c)], ssem.at[c, i]) for src, dst, i in pairs]

    def norm_and_gather(src, l, c, row, buf):
        for seq in (2 * c, 2 * c + 1):
            xhat, _ = normed(src[seq])
            val = xhat * vec[row, pl.ds(l, 1), :] + vec[row + 1, pl.ds(l, 1), :]
            buf[seq, pl.ds(0, 64)] = val.astype(BF)
            ex.gather(buf, seq).start()

    def first_copy(c):
        return ex.remote(x_in.at[seqs(c)], xbuf.at[seqs(c), pl.ds(32, 32)], isem.at[0, c], isem.at[1, c], 2)

    def position(axis):
        i = lax.broadcasted_iota(jnp.int32, (256, 128), axis) & 127
        block = ((i >> 6) & 1) | ((i >> 4) & 2)
        return ((block ^ ex.me) << 5) | (i & 31)

    def attention(c):
        a = rows_of(ag_a, c)
        for j in range(3):
            cols = pl.ds(512 * j, 512)
            qkv[seqs(c), :, cols] = dot_nt(a, wq[cols, :]).astype(BF).reshape(2, 128, 512)
        low = lane_low()

        @pl.loop(0, 2)
        def _(s):
            seq = 2 * c + s
            key_pos, query_pos = position(1), position(0)
            visible = (key_pos <= query_pos) & (key_pos < lens[seq])
            for pair in range(4):
                q, k, v = (qkv[seq, :, pl.ds(512 * t + 128 * pair, 128)] for t in range(3))
                scores = dot_nt(two_heads(q, low), k) * 0.125
                scores = jnp.where(visible, scores, -1e30)
                e = jnp.exp(scores - jnp.max(scores, axis=-1, keepdims=True))
                p = e / jnp.sum(e, axis=-1, keepdims=True)
                prob[seq, pair] = p
                pb = p.astype(BF)
                both = jnp.concatenate([pb[:128], pb[128:]], axis=1)
                ctx[seq, :, pl.ds(128 * pair, 128)] = dot_nn(both, two_heads(v, low)).astype(BF)

    def mlp(l, c):
        m = rows_of(ag_m, c)

        @pl.loop(0, 4)
        def _(j):
            cols = pl.ds(pl.multiple_of(512 * j, 512), 512)
            pre = dot_nn(m, wu[:, cols]) + bup[pl.ds(l, 1), cols]
            sq = pre * pre
            t = jnp.tanh(GELU_C * (pre + 0.044715 * (sq * pre)))
            grad = 0.5 * (1.0 + t) + 0.5 * pre * (1.0 - t * t) * (GELU_C * (1.0 + 0.134145 * sq))
            slope[seqs(c), :, cols] = grad.reshape(2, 128, 512)
            act[seqs(c), :, cols] = (0.5 * pre * (1.0 + t)).astype(BF).reshape(2, 128, 512)

    for kind in range(2):
        for copy in weight_copies(0, kind):
            copy.start()
    ex.barrier()
    for c in range(NUM_CHUNKS):
        first_copy(c).start()
    xbuf[:, pl.ds(0, 32)] = x_in[...]

    @pl.loop(0, n_layers)
    def _(l):
        for c in range(NUM_CHUNKS):
            @pl.when(l == 0)
            def _():
                first_copy(c).wait()

            @pl.when(l > 0)
            def _():
                xbuf[seqs(c)] = hbuf[seqs(c)] + ex.finish(1, c, True) + vec[5, pl.ds(l - 1, 1), :][None]

            norm_and_gather(xbuf, l, c, 0, ag_a)
            if c == 0:
                @pl.when(l > 0)
                def _():
                    ex.middle(1, 1, LAST, True)

                for copy in weight_copies(l, 0):
                    copy.wait()
            else:
                ex.middle(0, 0, LAST, True)
            ex.gather_wait(ag_a, c)
            attention(c)
            for copy in save_copies(l, c, 0):
                copy.start()
            lhs = rows_of(ctx, c)
            partial_sum(ex, 0, c, True, lambda cols: dot_nn(lhs, wo[:, cols]))

        @pl.when(l + 1 < n_layers)
        def _():
            for copy in weight_copies(l + 1, 0):
                copy.start()

        for c in range(NUM_CHUNKS):
            hbuf[seqs(c)] = xbuf[seqs(c)] + ex.finish(0, c, True) + vec[4, pl.ds(l, 1), :][None]
            norm_and_gather(hbuf, l, c, 2, ag_m)
            if c == 0:
                ex.middle(0, 1, LAST, True)
                for copy in weight_copies(l, 1):
                    copy.wait()
            else:
                ex.middle(1, 0, LAST, l + 1 < n_layers)
            ex.gather_wait(ag_m, c)
            mlp(l, c)
            for copy in save_copies(l, c, 1):
                copy.start()
            for copy in save_copies(l, c, 0):
                copy.wait()
            lhs = rows_of(act, c)
            partial_sum(ex, 1, c, l + 1 < n_layers, lambda cols: dot_nn(lhs, wd[:, cols]))

        @pl.when(l + 1 < n_layers)
        def _():
            for copy in weight_copies(l + 1, 1):
                copy.start()

        for c in range(NUM_CHUNKS):
            for copy in save_copies(l, c, 1):
                copy.wait()

    ex.middle(1, 1, LAST, False)
    for c in range(NUM_CHUNKS):
        y_out[seqs(c)] = hbuf[seqs(c), pl.ds(0, 32)] + ex.finish(1, c, False) + vec[5, pl.ds(n_layers - 1, 1), :][None]


def backward_kernel(dy_in, vec, wqkv_h, wout_h, wup_h, wdown_h, x_s, hid_s, qkv_s, p_s, slope_s,
                    d_x, dqkv_s, rhs_s, g_bup, g_vec,
                    wq, wo, wu, wd, dcur, dhid, zbuf, ag_a, ag_m, qkv, prob, slope, dpre, dctx, dqkv, vacc, vfar, vlast,
                    wsem, rsem, zsem, ssem, vsem, isem, part, from_core, far_send, far_recv, *sems):
    n_layers = wqkv_h.shape[0]
    ex = Exchange(part, from_core, far_send, far_recv, sems)

    def loads(l, kind):
        if kind == 0:
            whole = ((wqkv_h, wq, 0), (wout_h, wo, 1))
            saved = ((qkv_s, qkv, 1), (p_s, prob, 2))
        else:
            whole = ((wdown_h, wd, 3), (wup_h, wu, 2))
            saved = ((slope_s, slope, 0),)
        return ([pltpu.make_async_copy(src.at[l], dst, wsem.at[i]) for src, dst, i in whole]
                + [pltpu.make_async_copy(src.at[l], dst, rsem.at[i]) for src, dst, i in saved])

    def z_load(l, c, kind):
        return pltpu.make_async_copy((x_s, hid_s)[kind].at[l, seqs(c)], zbuf.at[seqs(c)], zsem.at[c])

    def save_copies(l, c, kind):
        pairs = ((ag_a, rhs_s.at[2], 0), (dqkv, dqkv_s, 1)) if kind == 0 else ((ag_m, rhs_s.at[1], 2), (dpre, rhs_s.at[0], 3))
        return [pltpu.make_async_copy(src.at[seqs(c)], dst.at[l, seqs(c)], ssem.at[c, i]) for src, dst, i in pairs]

    def send(src, c, buf):
        for seq in (2 * c, 2 * c + 1):
            buf[seq, pl.ds(0, 64)] = src[seq].astype(BF)
            ex.gather(buf, seq).start()

    def first_copy(c):
        return ex.remote(dy_in.at[seqs(c)], far_recv.at[0, seqs(c), pl.ds(0, 32)], isem.at[0, c], isem.at[1, c], 2)

    def dx_copy(c):
        return pltpu.make_async_copy(dcur.at[seqs(c), pl.ds(0, 32)], d_x.at[seqs(c)], isem.at[0, c])

    def row_sum(val):
        sums = [jnp.sum(val[:, 32 * i:32 * i + 32].reshape(64, -1), axis=0, keepdims=True) for i in range(val.shape[1] // 32)]
        return sums[0] if len(sums) == 1 else sums[0] + sums[1]

    def add_row(i, l, c, val):
        row = (i, pl.ds(l, 1))
        total = row_sum(val)
        vacc[row] = total if c == 0 else vacc[row] + total

    def norm_bwd(z, d_z, gain):
        shape = z.shape
        z, d_z = z.reshape(-1, shape[-1]), d_z.reshape(-1, shape[-1])
        xhat, rstd = normed(z)
        g = d_z * gain
        g_mean = jnp.mean(g, axis=-1, keepdims=True)
        gx_mean = jnp.mean(g * xhat, axis=-1, keepdims=True)
        return (rstd * (g - g_mean - xhat * gx_mean)).reshape(shape), (d_z * xhat).reshape(shape)

    def mlp_bwd(l, c):
        d_mlp = rows_of(ag_m, c)

        @pl.loop(0, 4)
        def _(j):
            cols = pl.ds(pl.multiple_of(512 * j, 512), 512)
            d_act = dot_nt(d_mlp, wd[cols, :]).astype(BF).astype(F32)
            d_pre = d_act * slope[seqs(c), :, cols].reshape(256, 512)
            total = jnp.sum(d_pre, axis=0, keepdims=True)
            g_bup[pl.ds(l, 1), cols] = total if c == 0 else g_bup[pl.ds(l, 1), cols] + total
            dpre[seqs(c), :, cols] = d_pre.astype(BF).reshape(2, 128, 512)

    def attention_bwd(c):
        dctx[seqs(c)] = dot_nt(rows_of(ag_a, c), wo[...]).astype(BF).reshape(2, 128, 512)
        low = lane_low()

        @pl.loop(0, 2)
        def _(s):
            seq = 2 * c + s
            for pair in range(4):
                q, k, v = (qkv[seq, :, pl.ds(512 * t + 128 * pair, 128)] for t in range(3))
                d_c = two_heads(dctx[seq, :, pl.ds(128 * pair, 128)], low)
                p = prob[seq, pair]
                d_p = dot_nt(d_c, v).astype(BF).astype(F32)
                d_s = p * (d_p - jnp.sum(d_p * p, axis=-1, keepdims=True))
                d_s = (d_s * 0.125).astype(BF)
                both = jnp.concatenate([d_s[:128], d_s[128:]], axis=1)
                d_q = dot_nn(both, two_heads(k, low))
                d_k = dot_tn(d_s, two_heads(q, low))
                d_v = dot_tn(p.astype(BF), d_c)
                for t, val in enumerate((d_q, d_k, d_v)):
                    dqkv[seq, :, pl.ds(512 * t + 128 * pair, 128)] = val.astype(BF)

    last = n_layers - 1
    for kind in (1, 0):
        for copy in loads(last, kind):
            copy.start()
    for c in range(NUM_CHUNKS):
        z_load(last, c, 1).start()
    ex.barrier()
    for c in range(NUM_CHUNKS):
        first_copy(c).start()
    dcur[:, pl.ds(0, 32)] = dy_in[...].astype(F32)

    @pl.loop(0, n_layers)
    def _(i):
        l = last - i

        for c in range(NUM_CHUNKS):
            @pl.when(i == 0)
            def _():
                first_copy(c).wait()
                dcur[seqs(c), pl.ds(32, 32)] = far_recv[0, seqs(c), pl.ds(0, 32)].astype(F32)

            @pl.when(i > 0)
            def _():
                d_in = ex.finish(0, c, True)
                z_load(l + 1, c, 0).wait()
                d_ln, d_gain = norm_bwd(zbuf[seqs(c)], d_in, vec[0, pl.ds(l + 1, 1), :])
                z_load(l, c, 1).start()
                dcur[seqs(c)] = dhid[seqs(c)] + d_ln
                send(dcur, c, ag_m)
                if c == 0:
                    ex.middle(0, 1, LAST, True)
                add_row(0, l + 1, c, d_gain)
                add_row(1, l + 1, c, d_in)

            @pl.when(i == 0)
            def _():
                send(dcur, c, ag_m)

            if c == 1:
                ex.middle(1, 0, LAST, True)
            add_row(5, l, c, dcur[seqs(c)])
            if c == 0:
                for copy in loads(l, 1):
                    copy.wait()
            ex.gather_wait(ag_m, c)
            mlp_bwd(l, c)
            for copy in save_copies(l, c, 1):
                copy.start()

            @pl.when(i > 0)
            def _():
                for copy in save_copies(l + 1, c, 0):
                    copy.wait()

            lhs = rows_of(dpre, c)
            partial_sum(ex, 1, c, True, lambda cols: dot_nt(lhs, wu[cols, :]))

        for c in range(NUM_CHUNKS):
            d_mid = ex.finish(1, c, True)
            z_load(l, c, 1).wait()
            d_ln, d_gain = norm_bwd(zbuf[seqs(c)], d_mid, vec[2, pl.ds(l, 1), :])
            z_load(l, c, 0).start()
            dhid[seqs(c)] = dcur[seqs(c)] + d_ln
            send(dhid, c, ag_a)
            if c == 0:
                ex.middle(1, 1, LAST, True)
            else:
                ex.middle(0, 0, LAST, l > 0)
            add_row(2, l, c, d_gain)
            add_row(3, l, c, d_mid)
            add_row(4, l, c, dhid[seqs(c)])
            if c == 0:
                for copy in loads(l, 0):
                    copy.wait()
            else:
                @pl.when(l > 0)
                def _():
                    for copy in loads(l - 1, 1):
                        copy.start()

            ex.gather_wait(ag_a, c)
            attention_bwd(c)
            for copy in save_copies(l, c, 0):
                copy.start()
            for copy in save_copies(l, c, 1):
                copy.wait()
            lhs = rows_of(dqkv, c)
            partial_sum(ex, 0, c, l > 0, lambda cols: dot_nn(lhs, wq[:, cols]))

        @pl.when(l > 0)
        def _():
            for copy in loads(l - 1, 0):
                copy.start()

    ex.middle(0, 1, LAST, False)
    for c in range(NUM_CHUNKS):
        z_load(0, c, 0).wait()
        for copy in save_copies(0, c, 0):
            copy.wait()
        d_in = ex.finish(0, c, False)
        d_ln, d_gain = norm_bwd(zbuf[seqs(c), pl.ds(0, 32)], d_in, vec[0, pl.ds(0, 1), :])
        dcur[seqs(c), pl.ds(0, 32)] = dhid[seqs(c), pl.ds(0, 32)] + d_ln
        dx_copy(c).start()
        for row, val in enumerate((d_gain, d_in)):
            total = row_sum(val)
            at = (0, pl.ds(row, 1))
            vlast[at] = total if c == 0 else vlast[at] + total
    copy = ex.remote(vlast.at[0], vlast.at[1], vsem.at[0, 0], vsem.at[0, 1], 2)
    copy.start()
    copy.wait()
    for row in range(2):
        vacc[row, pl.ds(0, 1)] = vlast[0, pl.ds(row, 1)] + vlast[1, pl.ds(row, 1)]
    copy = ex.remote(vacc, vfar, vsem.at[1, 0], vsem.at[1, 1], 1)
    copy.start()
    copy.wait()
    g_vec[...] = vacc[...] + vfar[...]
    for c in range(NUM_CHUNKS):
        dx_copy(c).wait()


def any_spec():
    return pl.BlockSpec(memory_space=pl.ANY)


def vmem_spec():
    return pl.BlockSpec(memory_space=pltpu.VMEM)


def run_forward(x, lens, vec, bup, wqkv, wout, wup, wdown):
    n, d = wqkv.shape[0], x.shape[-1]
    shape = jax.ShapeDtypeStruct
    dma = pltpu.SemaphoreType.DMA
    outs = [shape((4, 32, d), F32), shape((n, 4, 64, d), F32), shape((n, 4, 64, d), F32), shape((n, 4, 128, d), BF),
            shape((n, 4, 128, 1536), BF), shape((n, 4, 4, 256, 128), F32), shape((n, 4, 128, d), F32), shape((n, 4, 128, 2 * d + 512), BF)]
    return pl.pallas_call(
        forward_kernel,
        in_specs=[vmem_spec(), pl.BlockSpec(memory_space=pltpu.SMEM), vmem_spec(), vmem_spec()] + [any_spec()] * 4,
        out_specs=[vmem_spec()] + [any_spec()] * 7,
        out_shape=outs,
        scratch_shapes=[pltpu.VMEM((1536, d), BF), pltpu.VMEM((512, d), BF), pltpu.VMEM((d, d), BF), pltpu.VMEM((d, d), BF),
                        pltpu.VMEM((4, 64, d), F32), pltpu.VMEM((4, 64, d), F32), pltpu.VMEM((4, 128, d), BF), pltpu.VMEM((4, 128, d), BF),
                        pltpu.VMEM((4, 128, 1536), BF), pltpu.VMEM((4, 128, 512), BF), pltpu.VMEM((4, 4, 256, 128), F32),
                        pltpu.VMEM((4, 128, d), F32), pltpu.VMEM((4, 128, d), BF), dma((4,)), dma((2, 9)), dma((2, 2)), *Exchange.scratch(d)],
        compiler_params=pltpu.CompilerParams(collective_id=0, has_side_effects=True, vmem_limit_bytes=VMEM_LIMIT),
        name='forward',
    )(x, lens, vec, bup, wqkv, wout, wup, wdown)


def run_backward(dy, vec, wqkv, wout, wup, wdown, x_s, hid_s, qkv_s, p_s, slope_s):
    n, d = wqkv.shape[0], dy.shape[-1]
    shape = jax.ShapeDtypeStruct
    dma = pltpu.SemaphoreType.DMA
    outs = [shape((4, 32, d), F32), shape((n, 4, 128, 1536), BF), shape((3, n, 4, 128, d), BF), shape((n, d), F32), shape((6, n, d), F32)]
    return pl.pallas_call(
        backward_kernel,
        in_specs=[vmem_spec()] * 2 + [any_spec()] * 9,
        out_specs=[any_spec()] * 3 + [vmem_spec()] * 2,
        out_shape=outs,
        scratch_shapes=[pltpu.VMEM((1536, d), BF), pltpu.VMEM((512, d), BF), pltpu.VMEM((d, d), BF), pltpu.VMEM((d, d), BF)]
                       + [pltpu.VMEM((4, 64, d), F32)] * 3
                       + [pltpu.VMEM((4, 128, d), BF), pltpu.VMEM((4, 128, d), BF), pltpu.VMEM((4, 128, 1536), BF), pltpu.VMEM((4, 4, 256, 128), F32),
                          pltpu.VMEM((4, 128, d), F32), pltpu.VMEM((4, 128, d), BF), pltpu.VMEM((4, 128, 512), BF), pltpu.VMEM((4, 128, 1536), BF),
                          pltpu.VMEM((6, n, d), F32), pltpu.VMEM((6, n, d), F32), pltpu.VMEM((2, 2, d), F32),
                          dma((4,)), dma((3,)), dma((2,)), dma((2, 4)), dma((2, 2)), dma((2, 2)), *Exchange.scratch(d)],
        compiler_params=pltpu.CompilerParams(collective_id=1, has_side_effects=True, vmem_limit_bytes=VMEM_LIMIT),
        name='backward',
    )(dy, vec, wqkv, wout, wup, wdown, x_s, hid_s, qkv_s, p_s, slope_s)


def wgrad_kernel(lhs_f, lhs_b, rhs_f, rhs_b, g_up, g_down, g_qkv, g_out, lbuf, rbuf, obuf, lsem, rsem, osem):
    n, rows, d = rhs_f.shape
    kinds = ((lhs_f, 0, 1024, d // 1024, rhs_b.at[0], g_up), (lhs_f, d, 1024, d // 1024, rhs_b.at[1], g_down),
             (lhs_b, 0, 768, lhs_b.shape[2] // 768, rhs_f, g_qkv), (lhs_f, 2 * d, 512, (lhs_f.shape[2] - 2 * d) // 512, rhs_b.at[2], g_out))

    def lhs_copy(kind, s):
        src, first, tile, per, _, _ = kinds[kind]
        cols = pl.ds(pl.multiple_of(first + lax.rem(s, per) * tile, 128), tile)
        slot = lax.rem(s, 2)
        return pltpu.make_async_copy(src.at[s // per, :, cols], lbuf.at[slot, :, pl.ds(0, tile)], lsem.at[slot])

    def rhs_copy(kind, l):
        slot = lax.rem(l, 2)
        return pltpu.make_async_copy(kinds[kind][4].at[l], rbuf.at[slot], rsem.at[slot])

    def out_copy(kind, s):
        tile, per, out = kinds[kind][2], kinds[kind][3], kinds[kind][5]
        slot = lax.rem(s, 2)
        at = pl.ds(pl.multiple_of(lax.rem(s, per) * tile, 128), tile)
        return pltpu.make_async_copy(obuf.at[slot, pl.ds(0, tile)], out.at[s // per, at], osem.at[slot])

    lhs_copy(0, 0).start()
    rhs_copy(0, 0).start()
    for kind, (_, _, tile, per, _, _) in enumerate(kinds):
        steps = n * per

        @pl.loop(0, steps)
        def _(s):
            @pl.when(s + 1 < steps)
            def _():
                lhs_copy(kind, s + 1).start()

            @pl.when((lax.rem(s, per) == 0) & (s // per + 1 < n))
            def _():
                rhs_copy(kind, s // per + 1).start()

            if kind + 1 < len(kinds):
                @pl.when(s + 1 == steps)
                def _():
                    lhs_copy(kind + 1, 0).start()
                    rhs_copy(kind + 1, 0).start()

            lhs_copy(kind, s).wait()

            @pl.when(lax.rem(s, per) == 0)
            def _():
                rhs_copy(kind, s // per).wait()

            @pl.when(s >= 2)
            def _():
                out_copy(kind, s - 2).wait()

            if kind > 0:
                @pl.when(s < 2)
                def _():
                    out_copy(kind - 1, n * kinds[kind - 1][3] - 2 + s).wait()

            slot = lax.rem(s, 2)
            obuf[slot, pl.ds(0, tile)] = dot_tn(lbuf[slot, :, pl.ds(0, tile)], rbuf[lax.rem(s // per, 2)]).astype(BF)
            out_copy(kind, s).start()

    last = n * kinds[-1][3]
    for s in (last - 2, last - 1):
        out_copy(len(kinds) - 1, s).wait()


def weight_grads(lhs_f, lhs_b, rhs_f, rhs_b):
    n, rows, d = rhs_f.shape
    widths = (d, d, lhs_b.shape[2], lhs_f.shape[2] - 2 * d)
    dma = pltpu.SemaphoreType.DMA
    return pl.pallas_call(
        wgrad_kernel,
        in_specs=[any_spec()] * 4,
        out_specs=[any_spec()] * 4,
        out_shape=[jax.ShapeDtypeStruct((n, w, d), BF) for w in widths],
        scratch_shapes=[pltpu.VMEM((2, rows, 1024), BF), pltpu.VMEM((2, rows, d), BF), pltpu.VMEM((2, 1024, d), BF), dma((2,)), dma((2,)), dma((2,))],
        compiler_params=pltpu.CompilerParams(vmem_limit_bytes=52 * 1024 * 1024),
        cost_estimate=pl.CostEstimate(flops=2 * n * rows * d * sum(widths), bytes_accessed=2 * n * d * sum(widths), transcendentals=0),
        name='weight_grads',
    )(lhs_f, lhs_b, rhs_f, rhs_b)


def group_body(x_loc, dy_loc, len_loc, wqkv_loc, wout_loc, wup_loc, bup_loc, wdown_loc, vec_loc):
    n, d = wqkv_loc.shape[0], x_loc.shape[-1]
    vec = vec_loc.transpose(1, 0, 2)
    wqkv = wqkv_loc.transpose(0, 2, 3, 4, 1).reshape(n, 1536, d)
    wout = wout_loc.reshape(n, 512, d)
    y, x_s, hid_s, a_s, qkv_s, p_s, slope_s, lhs_s = run_forward(x_loc, len_loc, vec, bup_loc, wqkv, wout, wup_loc, wdown_loc)
    d_x, dqkv_s, rhs_s, g_bup, g_vec = run_backward(dy_loc, vec, wqkv, wout, wup_loc, wdown_loc, x_s, hid_s, qkv_s, p_s, slope_s)
    g_up, g_down, g_qkv, g_out = weight_grads(lhs_s.reshape(n, 512, -1), dqkv_s.reshape(n, 512, -1), a_s.reshape(n, 512, d), rhs_s.reshape(3, n, 512, d))
    g_qkv = g_qkv.reshape(n, 3, 8, 64, d).transpose(0, 4, 1, 2, 3)
    g_out = g_out.reshape(n, 8, 64, d)
    return y, d_x, g_qkv, g_out, g_up, g_bup, g_down, g_vec.transpose(1, 0, 2)


def solution(mesh):
    act_spec = P(PARTS_AXIS, TENSOR_AXIS, None)
    in_specs = (act_spec, act_spec, P(PARTS_AXIS), P(None, None, None, TENSOR_AXIS, None), P(None, TENSOR_AXIS, None, None), P(None, None, TENSOR_AXIS), P(None, TENSOR_AXIS), P(None, TENSOR_AXIS, None), P())
    out_specs = (act_spec, act_spec, P(PARTS_AXIS, None, None, TENSOR_AXIS, None), P(PARTS_AXIS, TENSOR_AXIS, None, None), P(PARTS_AXIS, None, TENSOR_AXIS), P(PARTS_AXIS, TENSOR_AXIS), P(PARTS_AXIS, TENSOR_AXIS, None), P(PARTS_AXIS, None, None))
    return jax.shard_map(group_body, mesh=mesh, in_specs=in_specs, out_specs=out_specs, check_vma=False)
```

```python
import functools
import jax
import jax.numpy as jnp
from jax import lax
from jax.experimental import pallas as pl
from jax.experimental.pallas import tpu as pltpu
from jax.sharding import PartitionSpec as P

TENSOR_AXIS = 'tp'
PARTS_AXIS = 'dp'
BF = jnp.bfloat16
F32 = jnp.float32
MESH = pl.DeviceIdType.MESH
VMEM_LIMIT = 67043328
SEQ = 128
HALF = 64
SHARD = 32
ROWS = 256
HEADS = 512
QKV = 3 * HEADS
TILE = 1024
BATCH = 4
TOKENS = BATCH * SEQ
NUM_CHUNKS = 2
RS_BLOCKS = 4
GELU_C = 0.7978845608028654


def dot_nn(a, b):
    return lax.dot_general(a, b, (((1,), (0,)), ((), ())), preferred_element_type=F32)


def dot_nt(a, b):
    return lax.dot_general(a, b, (((1,), (1,)), ((), ())), preferred_element_type=F32)


def dot_tn(a, b):
    return lax.dot_general(a, b, (((0,), (0,)), ((), ())), preferred_element_type=F32)


def seqs(c):
    return pl.ds(2 * c, 2)


def rows_of(ref, c):
    val = ref[seqs(c)]
    return val.reshape(ROWS, val.shape[-1])


def normed(z):
    mean = jnp.mean(z, axis=-1, keepdims=True)
    centered = z - mean
    var = jnp.mean(centered * centered, axis=-1, keepdims=True)
    rstd = lax.rsqrt(var + 1e-5)
    return centered * rstd, rstd


class Exchange:
    def __init__(self, part, from_core, far_send, far_recv, sems):
        self.me = lax.axis_index(TENSOR_AXIS)
        self.part, self.from_core = part, from_core
        self.far_send, self.far_recv = far_send, far_recv
        self.gs, self.gr, self.cs, self.cr, self.xs, self.xr = sems

    def remote(self, src, dst, send, recv, flip):
        return pltpu.make_async_remote_copy(
            src_ref=src, dst_ref=dst, send_sem=send, recv_sem=recv,
            device_id={TENSOR_AXIS: lax.bitwise_xor(self.me, flip)}, device_id_type=MESH)

    def barrier(self):
        sem = pltpu.get_barrier_semaphore()
        for flip in (1, 2):
            pl.semaphore_signal(sem, inc=1, device_id={TENSOR_AXIS: lax.bitwise_xor(self.me, flip)}, device_id_type=MESH)
        pl.semaphore_wait(sem, 2)

    def gather(self, buf, seq):
        return self.remote(buf.at[seq, pl.ds(0, HALF)], buf.at[seq, pl.ds(HALF, HALF)], self.gs.at[seq], self.gr.at[seq], 1)

    def gather_wait(self, buf, c):
        for s in range(2):
            self.gather(buf, 2 * c + s).wait()

    def cols(self, b):
        width = self.part.shape[-1] // RS_BLOCKS
        return pl.ds(pl.multiple_of(b * width, width), width)

    def core_copy(self, c, b):
        return self.remote(self.part.at[seqs(c), pl.ds(HALF, HALF), self.cols(b)], self.from_core.at[seqs(c), :, self.cols(b)],
                           self.cs.at[c, b], self.cr.at[c, b], 1)

    def far_copy(self, kind, c, b, full):
        rows = pl.ds(0, HALF) if full else pl.ds(SHARD, SHARD)
        return self.remote(self.far_send.at[seqs(c), rows, self.cols(b)], self.far_recv.at[kind, seqs(c), rows, self.cols(b)],
                           self.xs.at[kind, c, b], self.xr.at[kind, c, b], 2)

    def middle(self, kind, c, b, full=True):
        self.core_copy(c, b).wait_recv()
        near = self.part[seqs(c), pl.ds(0, HALF), self.cols(b)].astype(F32)
        self.far_send[seqs(c), :, self.cols(b)] = (near + self.from_core[seqs(c), :, self.cols(b)].astype(F32)).astype(BF)
        if isinstance(full, bool):
            self.far_copy(kind, c, b, full).start()
        else:
            @pl.when(full)
            def _():
                self.far_copy(kind, c, b, True).start()

            @pl.when(jnp.logical_not(full))
            def _():
                self.far_copy(kind, c, b, False).start()

    def finish(self, kind, c, full=True):
        for b in range(RS_BLOCKS):
            self.far_copy(kind, c, b, full).wait_recv()
            self.far_copy(kind, c, b, full).wait_send()
            self.core_copy(c, b).wait_send()
        own = self.far_send[seqs(c), pl.ds(0, SHARD)].astype(F32) + self.far_recv[kind, seqs(c), pl.ds(SHARD, SHARD)].astype(F32)
        own = own.astype(BF).astype(F32)
        if not full:
            return own
        twin = self.far_send[seqs(c), pl.ds(SHARD, SHARD)].astype(F32) + self.far_recv[kind, seqs(c), pl.ds(0, SHARD)].astype(F32)
        return jnp.concatenate([own, twin.astype(BF).astype(F32)], axis=1)

    @staticmethod
    def scratch(d):
        dma = pltpu.SemaphoreType.DMA
        return [pltpu.VMEM((BATCH, SEQ, d), BF), pltpu.VMEM((BATCH, HALF, d), BF), pltpu.VMEM((BATCH, HALF, d), BF), pltpu.VMEM((2, 4, HALF, d), BF),
                dma((4,)), dma((4,)), dma((2, RS_BLOCKS)), dma((2, RS_BLOCKS)), dma((2, 2, RS_BLOCKS)), dma((2, 2, RS_BLOCKS))]


LAST = RS_BLOCKS - 1


def partial_sum(ex, kind, c, block_of, full=True):
    @pl.loop(0, RS_BLOCKS)
    def _(b):
        cols = ex.cols(b)
        ex.part[seqs(c), :, cols] = block_of(cols).astype(BF).reshape(2, SEQ, -1)
        ex.core_copy(c, b).start()

        @pl.when(b > 0)
        def _():
            ex.middle(kind, c, b - 1, full)


def lane_low():
    return lax.broadcasted_iota(jnp.int32, (SEQ, SEQ), 1) < HALF


def two_heads(val, low):
    zero = jnp.zeros_like(val)
    return jnp.concatenate([jnp.where(low, val, zero), jnp.where(low, zero, val)], axis=0)


def stack_kernel(x_in, dy_in, lens, vec, bup, wqkv_h, wout_h, wup_h, wdown_h,
                 y_out, d_x, x_s, hid_s, a_s, qkv_s, p_s, slope_s, lhs_s, dqkv_s, rhs_s, g_bup, g_vec,
                 wq, wo, wu, wd, xbuf, hbuf, dcur, ag_a, ag_m, qkv, ctx, prob, slope, act, dqkv, dyfar, vacc, vfar, vlast,
                 wsem, ssem, isem, rsem, zsem, vsem, part, from_core, far_send, far_recv, *sems):
    n_layers = wqkv_h.shape[0]
    last = n_layers - 1
    ex = Exchange(part, from_core, far_send, far_recv, sems)

    d = x_in.shape[-1]

    def lhs_cols(start, width):
        return lhs_s.at[:, :, :, pl.ds(start, width)]

    def weight_copies(l, kind):
        pairs = ((wqkv_h, wq, 0), (wout_h, wo, 1)) if kind == 0 else ((wup_h, wu, 2), (wdown_h, wd, 3))
        return [pltpu.make_async_copy(src.at[l], dst, wsem.at[i]) for src, dst, i in pairs]

    def fwd_saves(l, c, kind):
        if kind == 0:
            pairs = ((xbuf, x_s, 0), (ag_a, a_s, 1), (qkv, qkv_s, 2), (ctx, lhs_cols(2 * d, HEADS), 3), (prob, p_s, 4))
        else:
            pairs = ((hbuf, hid_s, 5), (ag_m, lhs_cols(0, d), 6), (slope, slope_s, 7), (act, lhs_cols(d, d), 8))
        return [pltpu.make_async_copy(src.at[seqs(c)], dst.at[l, seqs(c)], ssem.at[c, i]) for src, dst, i in pairs]

    def norm_and_gather(src, l, c, row, buf):
        for seq in (2 * c, 2 * c + 1):
            xhat, _ = normed(src[seq])
            val = xhat * vec[row, pl.ds(l, 1), :] + vec[row + 1, pl.ds(l, 1), :]
            buf[seq, pl.ds(0, HALF)] = val.astype(BF)
            ex.gather(buf, seq).start()

    def dy_copy(c):
        return ex.remote(dy_in.at[seqs(c)], dyfar.at[seqs(c)], isem.at[2, c], isem.at[3, c], 2)

    def first_copy(c):
        return ex.remote(xbuf.at[seqs(c), pl.ds(0, SHARD)], xbuf.at[seqs(c), pl.ds(SHARD, SHARD)], isem.at[0, c], isem.at[1, c], 2)

    def position(axis):
        i = lax.broadcasted_iota(jnp.int32, (ROWS, SEQ), axis) & 127
        block = ((i >> 6) & 1) | ((i >> 4) & 2)
        return ((block ^ ex.me) << 5) | (i & 31)

    def attention(c):
        a = rows_of(ag_a, c)
        for j in range(3):
            cols = pl.ds(HEADS * j, HEADS)
            qkv[seqs(c), :, cols] = dot_nt(a, wq[cols, :]).astype(BF).reshape(2, SEQ, HEADS)
        low = lane_low()

        @pl.loop(0, 2)
        def _(s):
            seq = 2 * c + s
            key_pos, query_pos = position(1), position(0)
            visible = (key_pos <= query_pos) & (key_pos < lens[seq])
            for pair in range(4):
                q, k, v = (qkv[seq, :, pl.ds(HEADS * t + SEQ * pair, SEQ)] for t in range(3))
                scores = dot_nt(two_heads(q, low), k) * 0.125
                scores = jnp.where(visible, scores, -1e30)
                e = jnp.exp(scores - jnp.max(scores, axis=-1, keepdims=True))
                p = e / jnp.sum(e, axis=-1, keepdims=True)
                prob[seq, pair] = p
                pb = p.astype(BF)
                both = jnp.concatenate([pb[:SEQ], pb[SEQ:]], axis=1)
                ctx[seq, :, pl.ds(SEQ * pair, SEQ)] = dot_nn(both, two_heads(v, low)).astype(BF)

    def mlp(l, c):
        m = rows_of(ag_m, c)

        @pl.loop(0, 4)
        def _(j):
            cols = pl.ds(pl.multiple_of(HEADS * j, HEADS), HEADS)
            pre = dot_nn(m, wu[:, cols]) + bup[pl.ds(l, 1), cols]
            sq = pre * pre
            t = jnp.tanh(GELU_C * (pre + 0.044715 * (sq * pre)))
            grad = 0.5 * (1.0 + t) + 0.5 * pre * (1.0 - t * t) * (GELU_C * (1.0 + 0.134145 * sq))
            slope[seqs(c), :, cols] = grad.reshape(2, SEQ, HEADS)
            act[seqs(c), :, cols] = (0.5 * pre * (1.0 + t)).astype(BF).reshape(2, SEQ, HEADS)

    def loads(l, kind):
        if kind == 0:
            whole = ((wqkv_h, wq, 0), (wout_h, wo, 1))
            saved = ((qkv_s, qkv, 1), (p_s, prob, 2))
        else:
            whole = ((wdown_h, wd, 3), (wup_h, wu, 2))
            saved = ((slope_s, slope, 0),)
        return ([pltpu.make_async_copy(src.at[l], dst, wsem.at[i]) for src, dst, i in whole]
                + [pltpu.make_async_copy(src.at[l], dst, rsem.at[i]) for src, dst, i in saved])

    def z_load(l, c, kind):
        return pltpu.make_async_copy((x_s, hid_s)[kind].at[l, seqs(c)], xbuf.at[seqs(c)], zsem.at[c])

    def bwd_saves(l, c, kind):
        pairs = ((ag_a, rhs_s.at[2], 0), (dqkv, dqkv_s, 1)) if kind == 0 else ((ag_m, rhs_s.at[1], 2), (act, rhs_s.at[0], 3))
        return [pltpu.make_async_copy(src.at[seqs(c)], dst.at[l, seqs(c)], ssem.at[c, i]) for src, dst, i in pairs]

    def send(src, c, buf):
        for seq in (2 * c, 2 * c + 1):
            buf[seq, pl.ds(0, HALF)] = src[seq].astype(BF)
            ex.gather(buf, seq).start()

    def y_copy(c):
        return pltpu.make_async_copy(hbuf.at[seqs(c), pl.ds(0, SHARD)], y_out.at[seqs(c)], isem.at[1, c])

    def dx_copy(c):
        return pltpu.make_async_copy(dcur.at[seqs(c), pl.ds(0, SHARD)], d_x.at[seqs(c)], isem.at[0, c])

    def row_sum(val):
        sums = [jnp.sum(val[:, SHARD * i:SHARD * i + SHARD].reshape(HALF, -1), axis=0, keepdims=True) for i in range(val.shape[1] // SHARD)]
        return sums[0] if len(sums) == 1 else sums[0] + sums[1]

    def add_row(i, l, c, val):
        row = (i, pl.ds(l, 1))
        total = row_sum(val)
        vacc[row] = total if c == 0 else vacc[row] + total

    def norm_bwd(z, d_z, gain):
        shape = z.shape
        z, d_z = z.reshape(-1, shape[-1]), d_z.reshape(-1, shape[-1])
        xhat, rstd = normed(z)
        g = d_z * gain
        g_mean = jnp.mean(g, axis=-1, keepdims=True)
        gx_mean = jnp.mean(g * xhat, axis=-1, keepdims=True)
        return (rstd * (g - g_mean - xhat * gx_mean)).reshape(shape), (d_z * xhat).reshape(shape)

    def mlp_bwd(l, c):
        d_mlp = rows_of(ag_m, c)

        @pl.loop(0, 4)
        def _(j):
            cols = pl.ds(pl.multiple_of(HEADS * j, HEADS), HEADS)
            d_act = dot_nt(d_mlp, wd[cols, :]).astype(BF).astype(F32)
            d_pre = d_act * slope[seqs(c), :, cols].reshape(ROWS, HEADS)
            total = jnp.sum(d_pre, axis=0, keepdims=True)
            g_bup[pl.ds(l, 1), cols] = total if c == 0 else g_bup[pl.ds(l, 1), cols] + total
            act[seqs(c), :, cols] = d_pre.astype(BF).reshape(2, SEQ, HEADS)

    def attention_bwd(c):
        ctx[seqs(c)] = dot_nt(rows_of(ag_a, c), wo[...]).astype(BF).reshape(2, SEQ, HEADS)
        low = lane_low()

        @pl.loop(0, 2)
        def _(s):
            seq = 2 * c + s
            for pair in range(4):
                q, k, v = (qkv[seq, :, pl.ds(HEADS * t + SEQ * pair, SEQ)] for t in range(3))
                d_c = two_heads(ctx[seq, :, pl.ds(SEQ * pair, SEQ)], low)
                p = prob[seq, pair]
                d_p = dot_nt(d_c, v).astype(BF).astype(F32)
                d_s = p * (d_p - jnp.sum(d_p * p, axis=-1, keepdims=True))
                d_s = (d_s * 0.125).astype(BF)
                both = jnp.concatenate([d_s[:SEQ], d_s[SEQ:]], axis=1)
                d_q = dot_nn(both, two_heads(k, low))
                d_k = dot_tn(d_s, two_heads(q, low))
                d_v = dot_tn(p.astype(BF), d_c)
                for t, val in enumerate((d_q, d_k, d_v)):
                    dqkv[seq, :, pl.ds(HEADS * t + SEQ * pair, SEQ)] = val.astype(BF)

    x_copies = [pltpu.make_async_copy(x_in.at[seqs(c)], xbuf.at[seqs(c), pl.ds(0, SHARD)], isem.at[2, c]) for c in range(NUM_CHUNKS)]
    for copy in x_copies:
        copy.start()
    for kind in range(2):
        for copy in weight_copies(0, kind):
            copy.start()
    ex.barrier()
    for c in range(NUM_CHUNKS):
        x_copies[c].wait()
        first_copy(c).start()

    @pl.loop(0, n_layers)
    def _(l):
        for c in range(NUM_CHUNKS):
            @pl.when(l == 0)
            def _():
                first_copy(c).wait()

            @pl.when(l > 0)
            def _():
                xbuf[seqs(c)] = hbuf[seqs(c)] + ex.finish(1, c) + vec[5, pl.ds(l - 1, 1), :][None]

            norm_and_gather(xbuf, l, c, 0, ag_a)
            if c == 0:
                @pl.when(l > 0)
                def _():
                    ex.middle(1, 1, LAST)

                for copy in weight_copies(l, 0):
                    copy.wait()
            else:
                ex.middle(0, 0, LAST)
            ex.gather_wait(ag_a, c)
            attention(c)
            for copy in fwd_saves(l, c, 0):
                copy.start()
            lhs = rows_of(ctx, c)
            partial_sum(ex, 0, c, lambda cols: dot_nn(lhs, wo[:, cols]))

        @pl.when(l + 1 < n_layers)
        def _():
            for copy in weight_copies(l + 1, 0):
                copy.start()

        for c in range(NUM_CHUNKS):
            hbuf[seqs(c)] = xbuf[seqs(c)] + ex.finish(0, c) + vec[4, pl.ds(l, 1), :][None]
            norm_and_gather(hbuf, l, c, 2, ag_m)
            if c == 0:
                ex.middle(0, 1, LAST)

                @pl.when(l == last)
                def _():
                    for other in range(NUM_CHUNKS):
                        dy_copy(other).start()

                for copy in weight_copies(l, 1):
                    copy.wait()
            else:
                ex.middle(1, 0, LAST, l + 1 < n_layers)
            ex.gather_wait(ag_m, c)
            mlp(l, c)
            for copy in fwd_saves(l, c, 1):
                copy.start()
            for copy in fwd_saves(l, c, 0):
                copy.wait()
            lhs = rows_of(act, c)
            if c == 1:
                for copy in fwd_saves(l, 0, 1):
                    copy.wait()
            partial_sum(ex, 1, c, lambda cols: dot_nn(lhs, wd[:, cols]), l + 1 < n_layers)

        @pl.when(l + 1 < n_layers)
        def _():
            for copy in weight_copies(l + 1, 1):
                copy.start()

        for copy in fwd_saves(l, 1, 1):
            copy.wait()

    ex.middle(1, 1, LAST, False)
    for c in range(NUM_CHUNKS):
        z_load(last, c, 1).start()
    dcur[:, pl.ds(0, SHARD)] = dy_in[...].astype(F32)

    @pl.loop(0, n_layers)
    def _(i):
        l = last - i

        for c in range(NUM_CHUNKS):
            @pl.when(i == 0)
            def _():
                dy_copy(c).wait()
                dcur[seqs(c), pl.ds(SHARD, SHARD)] = dyfar[seqs(c)].astype(F32)
                send(dcur, c, ag_m)

            @pl.when(i > 0)
            def _():
                d_in = ex.finish(1, c)
                z_load(l + 1, c, 0).wait()
                d_ln, d_gain = norm_bwd(xbuf[seqs(c)], d_in, vec[0, pl.ds(l + 1, 1), :])
                z_load(l, c, 1).start()
                dcur[seqs(c)] = hbuf[seqs(c)] + d_ln
                send(dcur, c, ag_m)
                if c == 0:
                    ex.middle(1, 1, LAST)
                add_row(0, l + 1, c, d_gain)
                add_row(1, l + 1, c, d_in)

            if c == 1:
                ex.middle(0, 0, LAST)
            add_row(5, l, c, dcur[seqs(c)])
            if c == 0:
                @pl.when(i > 0)
                def _():
                    for copy in loads(l, 1):
                        copy.wait()

            ex.gather_wait(ag_m, c)
            mlp_bwd(l, c)
            for copy in bwd_saves(l, c, 1):
                copy.start()

            @pl.when(i > 0)
            def _():
                for copy in bwd_saves(l + 1, c, 0):
                    copy.wait()

            @pl.when(i == 0)
            def _():
                own = pl.ds(0, SHARD)
                hbuf[seqs(c), own] = hbuf[seqs(c), own] + ex.finish(1, c, False) + vec[5, pl.ds(last, 1), :][None]
                y_copy(c).start()

            lhs = rows_of(act, c)
            partial_sum(ex, 0, c, lambda cols: dot_nt(lhs, wu[cols, :]))

        for c in range(NUM_CHUNKS):
            d_mid = ex.finish(0, c)
            z_load(l, c, 1).wait()
            d_ln, d_gain = norm_bwd(xbuf[seqs(c)], d_mid, vec[2, pl.ds(l, 1), :])
            z_load(l, c, 0).start()

            @pl.when(i == 0)
            def _():
                y_copy(c).wait()

            hbuf[seqs(c)] = dcur[seqs(c)] + d_ln
            send(hbuf, c, ag_a)
            if c == 0:
                ex.middle(0, 1, LAST)
            else:
                ex.middle(1, 0, LAST, l > 0)
            add_row(2, l, c, d_gain)
            add_row(3, l, c, d_mid)
            add_row(4, l, c, hbuf[seqs(c)])
            if c == 0:
                @pl.when(i > 0)
                def _():
                    for copy in loads(l, 0):
                        copy.wait()
            else:
                @pl.when(l > 0)
                def _():
                    for copy in loads(l - 1, 1):
                        copy.start()

            ex.gather_wait(ag_a, c)
            attention_bwd(c)
            for copy in bwd_saves(l, c, 0):
                copy.start()
            for copy in bwd_saves(l, c, 1):
                copy.wait()
            lhs = rows_of(dqkv, c)
            partial_sum(ex, 1, c, lambda cols: dot_nn(lhs, wq[:, cols]), l > 0)

        @pl.when(l > 0)
        def _():
            for copy in loads(l - 1, 0):
                copy.start()

    ex.middle(1, 1, LAST, False)
    for c in range(NUM_CHUNKS):
        z_load(0, c, 0).wait()
        for copy in bwd_saves(0, c, 0):
            copy.wait()
        d_in = ex.finish(1, c, False)
        d_ln, d_gain = norm_bwd(xbuf[seqs(c), pl.ds(0, SHARD)], d_in, vec[0, pl.ds(0, 1), :])
        dcur[seqs(c), pl.ds(0, SHARD)] = hbuf[seqs(c), pl.ds(0, SHARD)] + d_ln
        dx_copy(c).start()
        for row, val in enumerate((d_gain, d_in)):
            total = row_sum(val)
            at = (0, pl.ds(row, 1))
            vlast[at] = total if c == 0 else vlast[at] + total
    copy = ex.remote(vlast.at[0], vlast.at[1], vsem.at[0, 0], vsem.at[0, 1], 2)
    copy.start()
    copy.wait()
    for row in range(2):
        vacc[row, pl.ds(0, 1)] = vlast[0, pl.ds(row, 1)] + vlast[1, pl.ds(row, 1)]
    copy = ex.remote(vacc, vfar, vsem.at[1, 0], vsem.at[1, 1], 1)
    copy.start()
    copy.wait()
    g_vec[...] = vacc[...] + vfar[...]
    for c in range(NUM_CHUNKS):
        dx_copy(c).wait()


def any_spec():
    return pl.BlockSpec(memory_space=pl.ANY)


def vmem_spec():
    return pl.BlockSpec(memory_space=pltpu.VMEM)


def run_stack(x, dy, lens, vec, bup, wqkv, wout, wup, wdown):
    n, d = wqkv.shape[0], x.shape[-1]
    shape = jax.ShapeDtypeStruct
    vmem = pltpu.VMEM
    dma = pltpu.SemaphoreType.DMA
    own, held, tokens = (BATCH, SHARD, d), (BATCH, HALF, d), (BATCH, SEQ, d)
    qkv, prob = (BATCH, SEQ, QKV), (BATCH, BATCH, ROWS, SEQ)
    outs = ([shape(own, F32)] * 2 + [shape((n, *held), F32)] * 2
            + [shape((n, *tokens), BF), shape((n, *qkv), BF), shape((n, *prob), F32), shape((n, *tokens), F32), shape((n, BATCH, SEQ, 2 * d + HEADS), BF),
               shape((n, *qkv), BF), shape((3, n, *tokens), BF), shape((n, d), F32), shape((6, n, d), F32)])
    scratch = ([vmem((QKV, d), BF), vmem((HEADS, d), BF), vmem((d, d), BF), vmem((d, d), BF)] + [vmem(held, F32)] * 3 + [vmem(tokens, BF)] * 2
               + [vmem(qkv, BF), vmem((BATCH, SEQ, HEADS), BF), vmem(prob, F32), vmem(tokens, F32), vmem(tokens, BF), vmem(qkv, BF), vmem(own, BF)]
               + [vmem((6, n, d), F32)] * 2 + [vmem((2, 2, d), F32)]
               + [dma((4,)), dma((2, 9)), dma((4, 2)), dma((3,)), dma((2,)), dma((2, 2))] + Exchange.scratch(d))
    return pl.pallas_call(
        stack_kernel,
        in_specs=[any_spec(), vmem_spec(), pl.BlockSpec(memory_space=pltpu.SMEM)] + [vmem_spec()] * 2 + [any_spec()] * 4,
        out_specs=[any_spec()] * 11 + [vmem_spec()] * 2,
        out_shape=outs,
        scratch_shapes=scratch,
        compiler_params=pltpu.CompilerParams(collective_id=0, has_side_effects=True, vmem_limit_bytes=VMEM_LIMIT),
        name='stack',
    )(x, dy, lens, vec, bup, wqkv, wout, wup, wdown)


def wgrad_kernel(lhs_f, lhs_b, rhs_f, rhs_b, g_up, g_down, g_qkv, g_out, lbuf, rbuf, obuf, lsem, rsem, osem):
    n, rows, d = rhs_f.shape
    kinds = ((lhs_f, 0, TILE, d // TILE, rhs_b.at[0], g_up), (lhs_f, d, TILE, d // TILE, rhs_b.at[1], g_down),
             (lhs_b, 0, 768, lhs_b.shape[2] // 768, rhs_f, g_qkv), (lhs_f, 2 * d, HEADS, (lhs_f.shape[2] - 2 * d) // HEADS, rhs_b.at[2], g_out))

    def lhs_copy(kind, s):
        src, first, tile, per, _, _ = kinds[kind]
        cols = pl.ds(pl.multiple_of(first + lax.rem(s, per) * tile, SEQ), tile)
        slot = lax.rem(s, 2)
        return pltpu.make_async_copy(src.at[s // per, :, cols], lbuf.at[slot, :, pl.ds(0, tile)], lsem.at[slot])

    def rhs_copy(kind, l):
        slot = lax.rem(l, 2)
        return pltpu.make_async_copy(kinds[kind][4].at[l], rbuf.at[slot], rsem.at[slot])

    def out_copy(kind, s):
        tile, per, out = kinds[kind][2], kinds[kind][3], kinds[kind][5]
        slot = lax.rem(s, 2)
        at = pl.ds(pl.multiple_of(lax.rem(s, per) * tile, SEQ), tile)
        return pltpu.make_async_copy(obuf.at[slot, pl.ds(0, tile)], out.at[s // per, at], osem.at[slot])

    lhs_copy(0, 0).start()
    rhs_copy(0, 0).start()
    for kind, (_, _, tile, per, _, _) in enumerate(kinds):
        steps = n * per

        @pl.loop(0, steps)
        def _(s):
            @pl.when(s + 1 < steps)
            def _():
                lhs_copy(kind, s + 1).start()

            @pl.when((lax.rem(s, per) == 0) & (s // per + 1 < n))
            def _():
                rhs_copy(kind, s // per + 1).start()

            if kind + 1 < len(kinds):
                @pl.when(s + 1 == steps)
                def _():
                    lhs_copy(kind + 1, 0).start()
                    rhs_copy(kind + 1, 0).start()

            lhs_copy(kind, s).wait()

            @pl.when(lax.rem(s, per) == 0)
            def _():
                rhs_copy(kind, s // per).wait()

            @pl.when(s >= 2)
            def _():
                out_copy(kind, s - 2).wait()

            if kind > 0:
                @pl.when(s < 2)
                def _():
                    out_copy(kind - 1, n * kinds[kind - 1][3] - 2 + s).wait()

            slot = lax.rem(s, 2)
            obuf[slot, pl.ds(0, tile)] = dot_tn(lbuf[slot, :, pl.ds(0, tile)], rbuf[lax.rem(s // per, 2)]).astype(BF)
            out_copy(kind, s).start()

    last = n * kinds[-1][3]
    for s in (last - 2, last - 1):
        out_copy(len(kinds) - 1, s).wait()


def weight_grads(lhs_f, lhs_b, rhs_f, rhs_b):
    n, rows, d = rhs_f.shape
    widths = (d, d, lhs_b.shape[2], lhs_f.shape[2] - 2 * d)
    dma = pltpu.SemaphoreType.DMA
    return pl.pallas_call(
        wgrad_kernel,
        in_specs=[any_spec()] * 4,
        out_specs=[any_spec()] * 4,
        out_shape=[jax.ShapeDtypeStruct((n, w, d), BF) for w in widths],
        scratch_shapes=[pltpu.VMEM((2, rows, TILE), BF), pltpu.VMEM((2, rows, d), BF), pltpu.VMEM((2, TILE, d), BF), dma((2,)), dma((2,)), dma((2,))],
        compiler_params=pltpu.CompilerParams(vmem_limit_bytes=52 * 1024 * 1024),
        cost_estimate=pl.CostEstimate(flops=2 * n * rows * d * sum(widths), bytes_accessed=2 * n * d * sum(widths), transcendentals=0),
        name='weight_grads',
    )(lhs_f, lhs_b, rhs_f, rhs_b)


def group_body(x_loc, dy_loc, len_loc, wqkv_loc, wout_loc, wup_loc, bup_loc, wdown_loc, vec_loc):
    n, d = wqkv_loc.shape[0], x_loc.shape[-1]
    vec = vec_loc.transpose(1, 0, 2)
    wqkv = wqkv_loc.transpose(0, 2, 3, 4, 1).reshape(n, QKV, d)
    wout = wout_loc.reshape(n, HEADS, d)
    outs = run_stack(x_loc, dy_loc, len_loc, vec, bup_loc, wqkv, wout, wup_loc, wdown_loc)
    y, d_x, _, _, a_s, _, _, _, lhs_s, dqkv_s, rhs_s, g_bup, g_vec = outs
    g_up, g_down, g_qkv, g_out = weight_grads(lhs_s.reshape(n, TOKENS, -1), dqkv_s.reshape(n, TOKENS, -1), a_s.reshape(n, TOKENS, d), rhs_s.reshape(3, n, TOKENS, d))
    g_qkv = g_qkv.reshape(n, 3, 8, HALF, d).transpose(0, 4, 1, 2, 3)
    g_out = g_out.reshape(n, 8, HALF, d)
    return y, d_x, g_qkv, g_out, g_up, g_bup, g_down, g_vec.transpose(1, 0, 2)


def solution(mesh):
    act_spec = P(PARTS_AXIS, TENSOR_AXIS, None)
    in_specs = (act_spec, act_spec, P(PARTS_AXIS), P(None, None, None, TENSOR_AXIS, None), P(None, TENSOR_AXIS, None, None), P(None, None, TENSOR_AXIS), P(None, TENSOR_AXIS), P(None, TENSOR_AXIS, None), P())
    out_specs = (act_spec, act_spec, P(PARTS_AXIS, None, None, TENSOR_AXIS, None), P(PARTS_AXIS, TENSOR_AXIS, None, None), P(PARTS_AXIS, None, TENSOR_AXIS), P(PARTS_AXIS, TENSOR_AXIS), P(PARTS_AXIS, TENSOR_AXIS, None), P(PARTS_AXIS, None, None))
    return jax.shard_map(group_body, mesh=mesh, in_specs=in_specs, out_specs=out_specs, check_vma=False)
```

```python
import functools
import jax
import jax.numpy as jnp
from jax import lax
from jax.experimental import pallas as pl
from jax.experimental.pallas import tpu as pltpu
from jax.sharding import PartitionSpec as P

TENSOR_AXIS = 'tp'
PARTS_AXIS = 'dp'
BF = jnp.bfloat16
F32 = jnp.float32
MESH = pl.DeviceIdType.MESH
VMEM_LIMIT = 67043328
SEQ = 128
HALF = 64
SHARD = 32
ROWS = 256
HEADS = 512
QKV = 3 * HEADS
TILE = 1024
BATCH = 4
TOKENS = BATCH * SEQ
NUM_CHUNKS = 2
RS_BLOCKS = 4
GELU_C = 0.7978845608028654


def dot_nn(a, b):
    return lax.dot_general(a, b, (((1,), (0,)), ((), ())), preferred_element_type=F32)


def dot_nt(a, b):
    return lax.dot_general(a, b, (((1,), (1,)), ((), ())), preferred_element_type=F32)


def dot_tn(a, b):
    return lax.dot_general(a, b, (((0,), (0,)), ((), ())), preferred_element_type=F32)


def seqs(c):
    return pl.ds(2 * c, 2)


def rows_of(ref, c):
    val = ref[seqs(c)]
    return val.reshape(ROWS, val.shape[-1])


def normed(z):
    mean = jnp.mean(z, axis=-1, keepdims=True)
    centered = z - mean
    var = jnp.mean(centered * centered, axis=-1, keepdims=True)
    rstd = lax.rsqrt(var + 1e-5)
    return centered * rstd, rstd


class Exchange:
    def __init__(self, part, from_core, far_send, far_recv, sems):
        self.me = lax.axis_index(TENSOR_AXIS)
        self.part, self.from_core = part, from_core
        self.far_send, self.far_recv = far_send, far_recv
        self.gs, self.gr, self.cs, self.cr, self.xs, self.xr = sems

    def remote(self, src, dst, send, recv, flip):
        return pltpu.make_async_remote_copy(
            src_ref=src, dst_ref=dst, send_sem=send, recv_sem=recv,
            device_id={TENSOR_AXIS: lax.bitwise_xor(self.me, flip)}, device_id_type=MESH)

    def barrier(self):
        sem = pltpu.get_barrier_semaphore()
        for flip in (1, 2):
            pl.semaphore_signal(sem, inc=1, device_id={TENSOR_AXIS: lax.bitwise_xor(self.me, flip)}, device_id_type=MESH)
        pl.semaphore_wait(sem, 2)

    def gather(self, buf, seq):
        return self.remote(buf.at[seq, pl.ds(0, HALF)], buf.at[seq, pl.ds(HALF, HALF)], self.gs.at[seq], self.gr.at[seq], 1)

    def gather_wait(self, buf, c):
        for s in range(2):
            self.gather(buf, 2 * c + s).wait()

    def cols(self, b):
        width = self.part.shape[-1] // RS_BLOCKS
        return pl.ds(pl.multiple_of(b * width, width), width)

    def core_copy(self, c, b):
        return self.remote(self.part.at[seqs(c), pl.ds(HALF, HALF), self.cols(b)], self.from_core.at[seqs(c), :, self.cols(b)],
                           self.cs.at[c, b], self.cr.at[c, b], 1)

    def far_copy(self, kind, c, b, full):
        rows = pl.ds(0, HALF) if full else pl.ds(SHARD, SHARD)
        return self.remote(self.far_send.at[seqs(c), rows, self.cols(b)], self.far_recv.at[kind, seqs(c), rows, self.cols(b)],
                           self.xs.at[kind, c, b], self.xr.at[kind, c, b], 2)

    def middle(self, kind, c, b, full=True):
        self.core_copy(c, b).wait_recv()
        near = self.part[seqs(c), pl.ds(0, HALF), self.cols(b)].astype(F32)
        self.far_send[seqs(c), :, self.cols(b)] = (near + self.from_core[seqs(c), :, self.cols(b)].astype(F32)).astype(BF)
        if isinstance(full, bool):
            self.far_copy(kind, c, b, full).start()
        else:
            @pl.when(full)
            def _():
                self.far_copy(kind, c, b, True).start()

            @pl.when(jnp.logical_not(full))
            def _():
                self.far_copy(kind, c, b, False).start()

    def finish(self, kind, c, full=True):
        for b in range(RS_BLOCKS):
            self.far_copy(kind, c, b, full).wait_recv()
            self.far_copy(kind, c, b, full).wait_send()
            self.core_copy(c, b).wait_send()
        own = self.far_send[seqs(c), pl.ds(0, SHARD)].astype(F32) + self.far_recv[kind, seqs(c), pl.ds(SHARD, SHARD)].astype(F32)
        own = own.astype(BF).astype(F32)
        if not full:
            return own
        twin = self.far_send[seqs(c), pl.ds(SHARD, SHARD)].astype(F32) + self.far_recv[kind, seqs(c), pl.ds(0, SHARD)].astype(F32)
        return jnp.concatenate([own, twin.astype(BF).astype(F32)], axis=1)

    @staticmethod
    def scratch(d):
        dma = pltpu.SemaphoreType.DMA
        return [pltpu.VMEM((BATCH, SEQ, d), BF), pltpu.VMEM((BATCH, HALF, d), BF), pltpu.VMEM((BATCH, HALF, d), BF), pltpu.VMEM((2, 4, HALF, d), BF),
                dma((4,)), dma((4,)), dma((2, RS_BLOCKS)), dma((2, RS_BLOCKS)), dma((2, 2, RS_BLOCKS)), dma((2, 2, RS_BLOCKS))]


LAST = RS_BLOCKS - 1


def partial_sum(ex, kind, c, block_of, full=True):
    @pl.loop(0, RS_BLOCKS)
    def _(b):
        cols = ex.cols(b)
        ex.part[seqs(c), :, cols] = block_of(cols).astype(BF).reshape(2, SEQ, -1)
        ex.core_copy(c, b).start()

        @pl.when(b > 0)
        def _():
            ex.middle(kind, c, b - 1, full)


def lane_low():
    return lax.broadcasted_iota(jnp.int32, (SEQ, SEQ), 1) < HALF


def two_heads(val, low):
    zero = jnp.zeros_like(val)
    return jnp.concatenate([jnp.where(low, val, zero), jnp.where(low, zero, val)], axis=0)


def stack_kernel(x_in, dy_in, lens, vec, bup, wqkv_h, wout_h, wup_h, wdown_h,
                 y_out, d_x, x_s, hid_s, a_s, qkv_s, p_s, slope_s, lhs_s, dqkv_s, rhs_s, g_bup, g_vec,
                 wq, wo, wu, wd, xbuf, hbuf, dcur, ag_a, ag_m, qkv, ctx, prob, slope, act, dqkv, dyfar, vacc, vfar, vlast,
                 wsem, ssem, isem, rsem, zsem, vsem, part, from_core, far_send, far_recv, *sems):
    n_layers = wqkv_h.shape[0]
    last = n_layers - 1
    ex = Exchange(part, from_core, far_send, far_recv, sems)

    d = x_in.shape[-1]

    def lhs_cols(start, width):
        return lhs_s.at[:, :, :, pl.ds(start, width)]

    def weight_copies(l, kind):
        pairs = ((wqkv_h, wq, 0), (wout_h, wo, 1)) if kind == 0 else ((wup_h, wu, 2), (wdown_h, wd, 3))
        return [pltpu.make_async_copy(src.at[l], dst, wsem.at[i]) for src, dst, i in pairs]

    def fwd_saves(l, c, kind):
        if kind == 0:
            pairs = ((xbuf, x_s, 0), (ag_a, a_s, 1), (qkv, qkv_s, 2), (ctx, lhs_cols(2 * d, HEADS), 3), (prob, p_s, 4))
        else:
            pairs = ((hbuf, hid_s, 5), (ag_m, lhs_cols(0, d), 6), (slope, slope_s, 7), (act, lhs_cols(d, d), 8))
        return [pltpu.make_async_copy(src.at[seqs(c)], dst.at[l, seqs(c)], ssem.at[c, i]) for src, dst, i in pairs]

    def norm_and_gather(src, l, c, row, buf):
        for seq in (2 * c, 2 * c + 1):
            xhat, _ = normed(src[seq])
            val = xhat * vec[row, pl.ds(l, 1), :] + vec[row + 1, pl.ds(l, 1), :]
            buf[seq, pl.ds(0, HALF)] = val.astype(BF)
            ex.gather(buf, seq).start()

    def dy_copy(c):
        return ex.remote(dy_in.at[seqs(c)], dyfar.at[seqs(c)], isem.at[2, c], isem.at[3, c], 2)

    def first_copy(c):
        return ex.remote(xbuf.at[seqs(c), pl.ds(0, SHARD)], xbuf.at[seqs(c), pl.ds(SHARD, SHARD)], isem.at[0, c], isem.at[1, c], 2)

    def position(axis):
        i = lax.broadcasted_iota(jnp.int32, (ROWS, SEQ), axis) & 127
        block = ((i >> 6) & 1) | ((i >> 4) & 2)
        return ((block ^ ex.me) << 5) | (i & 31)

    def attention(c):
        a = rows_of(ag_a, c)
        for j in range(3):
            cols = pl.ds(HEADS * j, HEADS)
            qkv[seqs(c), :, cols] = dot_nt(a, wq[cols, :]).astype(BF).reshape(2, SEQ, HEADS)
        low = lane_low()

        @pl.loop(0, 2)
        def _(s):
            seq = 2 * c + s
            key_pos, query_pos = position(1), position(0)
            visible = (key_pos <= query_pos) & (key_pos < lens[seq])
            for pair in range(4):
                q, k, v = (qkv[seq, :, pl.ds(HEADS * t + SEQ * pair, SEQ)] for t in range(3))
                scores = dot_nt(two_heads(q, low), k) * 0.125
                scores = jnp.where(visible, scores, -1e30)
                e = jnp.exp(scores - jnp.max(scores, axis=-1, keepdims=True))
                p = e / jnp.sum(e, axis=-1, keepdims=True)
                prob[seq, pair] = p
                pb = p.astype(BF)
                both = jnp.concatenate([pb[:SEQ], pb[SEQ:]], axis=1)
                ctx[seq, :, pl.ds(SEQ * pair, SEQ)] = dot_nn(both, two_heads(v, low)).astype(BF)

    def mlp(l, c):
        m = rows_of(ag_m, c)

        @pl.loop(0, 4)
        def _(j):
            cols = pl.ds(pl.multiple_of(HEADS * j, HEADS), HEADS)
            pre = dot_nn(m, wu[:, cols]) + bup[pl.ds(l, 1), cols]
            sq = pre * pre
            t = jnp.tanh(GELU_C * (pre + 0.044715 * (sq * pre)))
            grad = 0.5 * (1.0 + t) + 0.5 * pre * (1.0 - t * t) * (GELU_C * (1.0 + 0.134145 * sq))
            slope[seqs(c), :, cols] = grad.reshape(2, SEQ, HEADS)
            act[seqs(c), :, cols] = (0.5 * pre * (1.0 + t)).astype(BF).reshape(2, SEQ, HEADS)

    def loads(l, kind):
        if kind == 0:
            whole = ((wqkv_h, wq, 0), (wout_h, wo, 1))
            saved = ((qkv_s, qkv, 1), (p_s, prob, 2))
        else:
            whole = ((wdown_h, wd, 3), (wup_h, wu, 2))
            saved = ((slope_s, slope, 0),)
        return ([pltpu.make_async_copy(src.at[l], dst, wsem.at[i]) for src, dst, i in whole]
                + [pltpu.make_async_copy(src.at[l], dst, rsem.at[i]) for src, dst, i in saved])

    def z_load(l, c, kind):
        return pltpu.make_async_copy((x_s, hid_s)[kind].at[l, seqs(c)], xbuf.at[seqs(c)], zsem.at[c])

    def bwd_saves(l, c, kind):
        pairs = ((ag_a, rhs_s.at[2], 0), (dqkv, dqkv_s, 1)) if kind == 0 else ((ag_m, rhs_s.at[1], 2), (act, rhs_s.at[0], 3))
        return [pltpu.make_async_copy(src.at[seqs(c)], dst.at[l, seqs(c)], ssem.at[c, i]) for src, dst, i in pairs]

    def send(src, c, buf):
        for seq in (2 * c, 2 * c + 1):
            buf[seq, pl.ds(0, HALF)] = src[seq].astype(BF)
            ex.gather(buf, seq).start()

    def y_copy(c):
        return pltpu.make_async_copy(hbuf.at[seqs(c), pl.ds(0, SHARD)], y_out.at[seqs(c)], isem.at[1, c])

    def dx_copy(c):
        return pltpu.make_async_copy(dcur.at[seqs(c), pl.ds(0, SHARD)], d_x.at[seqs(c)], isem.at[0, c])

    def row_sum(val):
        sums = [jnp.sum(val[:, SHARD * i:SHARD * i + SHARD].reshape(HALF, -1), axis=0, keepdims=True) for i in range(val.shape[1] // SHARD)]
        return sums[0] if len(sums) == 1 else sums[0] + sums[1]

    def add_row(i, l, c, val):
        row = (i, pl.ds(l, 1))
        total = row_sum(val)
        vacc[row] = total if c == 0 else vacc[row] + total

    def norm_bwd(z, d_z, gain):
        shape = z.shape
        z, d_z = z.reshape(-1, shape[-1]), d_z.reshape(-1, shape[-1])
        xhat, rstd = normed(z)
        g = d_z * gain
        g_mean = jnp.mean(g, axis=-1, keepdims=True)
        gx_mean = jnp.mean(g * xhat, axis=-1, keepdims=True)
        return (rstd * (g - g_mean - xhat * gx_mean)).reshape(shape), (d_z * xhat).reshape(shape)

    def mlp_bwd(l, c):
        d_mlp = rows_of(ag_m, c)

        @pl.loop(0, 4)
        def _(j):
            cols = pl.ds(pl.multiple_of(HEADS * j, HEADS), HEADS)
            d_act = dot_nt(d_mlp, wd[cols, :]).astype(BF).astype(F32)
            d_pre = d_act * slope[seqs(c), :, cols].reshape(ROWS, HEADS)
            total = jnp.sum(d_pre, axis=0, keepdims=True)
            g_bup[pl.ds(l, 1), cols] = total if c == 0 else g_bup[pl.ds(l, 1), cols] + total
            act[seqs(c), :, cols] = d_pre.astype(BF).reshape(2, SEQ, HEADS)

    def attention_bwd(c):
        ctx[seqs(c)] = dot_nt(rows_of(ag_a, c), wo[...]).astype(BF).reshape(2, SEQ, HEADS)
        low = lane_low()

        @pl.loop(0, 2)
        def _(s):
            seq = 2 * c + s
            for pair in range(4):
                q, k, v = (qkv[seq, :, pl.ds(HEADS * t + SEQ * pair, SEQ)] for t in range(3))
                d_c = two_heads(ctx[seq, :, pl.ds(SEQ * pair, SEQ)], low)
                p = prob[seq, pair]
                d_p = dot_nt(d_c, v).astype(BF).astype(F32)
                d_s = p * (d_p - jnp.sum(d_p * p, axis=-1, keepdims=True))
                d_s = (d_s * 0.125).astype(BF)
                both = jnp.concatenate([d_s[:SEQ], d_s[SEQ:]], axis=1)
                d_q = dot_nn(both, two_heads(k, low))
                d_k = dot_tn(d_s, two_heads(q, low))
                d_v = dot_tn(p.astype(BF), d_c)
                for t, val in enumerate((d_q, d_k, d_v)):
                    dqkv[seq, :, pl.ds(HEADS * t + SEQ * pair, SEQ)] = val.astype(BF)

    x_copies = [pltpu.make_async_copy(x_in.at[seqs(c)], xbuf.at[seqs(c), pl.ds(0, SHARD)], isem.at[2, c]) for c in range(NUM_CHUNKS)]
    for copy in x_copies:
        copy.start()
    for kind in range(2):
        for copy in weight_copies(0, kind):
            copy.start()
    ex.barrier()
    for c in range(NUM_CHUNKS):
        x_copies[c].wait()
        first_copy(c).start()

    @pl.loop(0, n_layers)
    def _(l):
        for c in range(NUM_CHUNKS):
            @pl.when(l == 0)
            def _():
                first_copy(c).wait()

            @pl.when(l > 0)
            def _():
                xbuf[seqs(c)] = hbuf[seqs(c)] + ex.finish(1, c) + vec[5, pl.ds(l - 1, 1), :][None]

            norm_and_gather(xbuf, l, c, 0, ag_a)
            if c == 0:
                @pl.when(l > 0)
                def _():
                    ex.middle(1, 1, LAST)

                for copy in weight_copies(l, 0):
                    copy.wait()
            else:
                ex.middle(0, 0, LAST)
            ex.gather_wait(ag_a, c)
            attention(c)
            for copy in fwd_saves(l, c, 0):
                copy.start()
            lhs = rows_of(ctx, c)
            partial_sum(ex, 0, c, lambda cols: dot_nn(lhs, wo[:, cols]))

        @pl.when(l + 1 < n_layers)
        def _():
            for copy in weight_copies(l + 1, 0):
                copy.start()

        for c in range(NUM_CHUNKS):
            hbuf[seqs(c)] = xbuf[seqs(c)] + ex.finish(0, c) + vec[4, pl.ds(l, 1), :][None]
            norm_and_gather(hbuf, l, c, 2, ag_m)
            if c == 0:
                ex.middle(0, 1, LAST)

                @pl.when(l == last)
                def _():
                    for other in range(NUM_CHUNKS):
                        dy_copy(other).start()

                for copy in weight_copies(l, 1):
                    copy.wait()
            else:
                ex.middle(1, 0, LAST, l + 1 < n_layers)
            ex.gather_wait(ag_m, c)
            mlp(l, c)
            for copy in fwd_saves(l, c, 1):
                copy.start()
            for copy in fwd_saves(l, c, 0):
                copy.wait()
            lhs = rows_of(act, c)
            if c == 1:
                for copy in fwd_saves(l, 0, 1):
                    copy.wait()
            partial_sum(ex, 1, c, lambda cols: dot_nn(lhs, wd[:, cols]), l + 1 < n_layers)

        @pl.when(l + 1 < n_layers)
        def _():
            for copy in weight_copies(l + 1, 1):
                copy.start()

        for copy in fwd_saves(l, 1, 1):
            copy.wait()

    ex.middle(1, 1, LAST, False)
    for c in range(NUM_CHUNKS):
        z_load(last, c, 1).start()
    dcur[:, pl.ds(0, SHARD)] = dy_in[...].astype(F32)

    @pl.loop(0, n_layers)
    def _(i):
        l = last - i

        for c in range(NUM_CHUNKS):
            @pl.when(i == 0)
            def _():
                dy_copy(c).wait()
                dcur[seqs(c), pl.ds(SHARD, SHARD)] = dyfar[seqs(c)].astype(F32)
                send(dcur, c, ag_m)

            @pl.when(i > 0)
            def _():
                d_in = ex.finish(1, c)
                z_load(l + 1, c, 0).wait()
                d_ln, d_gain = norm_bwd(xbuf[seqs(c)], d_in, vec[0, pl.ds(l + 1, 1), :])
                z_load(l, c, 1).start()
                dcur[seqs(c)] = hbuf[seqs(c)] + d_ln
                send(dcur, c, ag_m)
                if c == 0:
                    ex.middle(1, 1, LAST)
                add_row(0, l + 1, c, d_gain)
                add_row(1, l + 1, c, d_in)

            if c == 1:
                ex.middle(0, 0, LAST)
            add_row(5, l, c, dcur[seqs(c)])
            if c == 0:
                @pl.when(i > 0)
                def _():
                    for copy in loads(l, 1):
                        copy.wait()

            ex.gather_wait(ag_m, c)
            mlp_bwd(l, c)
            for copy in bwd_saves(l, c, 1):
                copy.start()

            @pl.when(i > 0)
            def _():
                for copy in bwd_saves(l + 1, c, 0):
                    copy.wait()

            @pl.when(i == 0)
            def _():
                own = pl.ds(0, SHARD)
                hbuf[seqs(c), own] = hbuf[seqs(c), own] + ex.finish(1, c, False) + vec[5, pl.ds(last, 1), :][None]
                y_copy(c).start()

            lhs = rows_of(act, c)
            partial_sum(ex, 0, c, lambda cols: dot_nt(lhs, wu[cols, :]))

        for c in range(NUM_CHUNKS):
            d_mid = ex.finish(0, c)
            z_load(l, c, 1).wait()
            d_ln, d_gain = norm_bwd(xbuf[seqs(c)], d_mid, vec[2, pl.ds(l, 1), :])
            z_load(l, c, 0).start()

            @pl.when(i == 0)
            def _():
                y_copy(c).wait()

            hbuf[seqs(c)] = dcur[seqs(c)] + d_ln
            send(hbuf, c, ag_a)
            if c == 0:
                ex.middle(0, 1, LAST)
            else:
                ex.middle(1, 0, LAST, l > 0)
            add_row(2, l, c, d_gain)
            add_row(3, l, c, d_mid)
            add_row(4, l, c, hbuf[seqs(c)])
            if c == 0:
                @pl.when(i > 0)
                def _():
                    for copy in loads(l, 0):
                        copy.wait()
            else:
                @pl.when(l > 0)
                def _():
                    for copy in loads(l - 1, 1):
                        copy.start()

            ex.gather_wait(ag_a, c)
            attention_bwd(c)
            for copy in bwd_saves(l, c, 0):
                copy.start()
            for copy in bwd_saves(l, c, 1):
                copy.wait()
            lhs = rows_of(dqkv, c)
            partial_sum(ex, 1, c, lambda cols: dot_nn(lhs, wq[:, cols]), l > 0)

        @pl.when(l > 0)
        def _():
            for copy in loads(l - 1, 0):
                copy.start()

    ex.middle(1, 1, LAST, False)
    for c in range(NUM_CHUNKS):
        z_load(0, c, 0).wait()
        for copy in bwd_saves(0, c, 0):
            copy.wait()
        d_in = ex.finish(1, c, False)
        d_ln, d_gain = norm_bwd(xbuf[seqs(c), pl.ds(0, SHARD)], d_in, vec[0, pl.ds(0, 1), :])
        dcur[seqs(c), pl.ds(0, SHARD)] = hbuf[seqs(c), pl.ds(0, SHARD)] + d_ln
        dx_copy(c).start()
        for row, val in enumerate((d_gain, d_in)):
            total = row_sum(val)
            at = (0, pl.ds(row, 1))
            vlast[at] = total if c == 0 else vlast[at] + total
    copy = ex.remote(vlast.at[0], vlast.at[1], vsem.at[0, 0], vsem.at[0, 1], 2)
    copy.start()
    copy.wait()
    for row in range(2):
        vacc[row, pl.ds(0, 1)] = vlast[0, pl.ds(row, 1)] + vlast[1, pl.ds(row, 1)]
    copy = ex.remote(vacc, vfar, vsem.at[1, 0], vsem.at[1, 1], 1)
    copy.start()
    copy.wait()
    g_vec[...] = vacc[...] + vfar[...]
    for c in range(NUM_CHUNKS):
        dx_copy(c).wait()


def any_spec():
    return pl.BlockSpec(memory_space=pl.ANY)


def vmem_spec():
    return pl.BlockSpec(memory_space=pltpu.VMEM)


def run_stack(x, dy, lens, vec, bup, wqkv, wout, wup, wdown):
    n, d = wqkv.shape[0], x.shape[-1]
    shape = jax.ShapeDtypeStruct
    vmem = pltpu.VMEM
    dma = pltpu.SemaphoreType.DMA
    own, held, tokens = (BATCH, SHARD, d), (BATCH, HALF, d), (BATCH, SEQ, d)
    qkv, prob = (BATCH, SEQ, QKV), (BATCH, BATCH, ROWS, SEQ)
    outs = ([shape(own, F32)] * 2 + [shape((n, *held), F32)] * 2
            + [shape((n, *tokens), BF), shape((n, *qkv), BF), shape((n, *prob), F32), shape((n, *tokens), F32), shape((n, BATCH, SEQ, 2 * d + HEADS), BF),
               shape((n, *qkv), BF), shape((3, n, *tokens), BF), shape((n, d), F32), shape((6, n, d), F32)])
    scratch = ([vmem((QKV, d), BF), vmem((HEADS, d), BF), vmem((d, d), BF), vmem((d, d), BF)] + [vmem(held, F32)] * 3 + [vmem(tokens, BF)] * 2
               + [vmem(qkv, BF), vmem((BATCH, SEQ, HEADS), BF), vmem(prob, F32), vmem(tokens, F32), vmem(tokens, BF), vmem(qkv, BF), vmem(own, BF)]
               + [vmem((6, n, d), F32)] * 2 + [vmem((2, 2, d), F32)]
               + [dma((4,)), dma((2, 9)), dma((4, 2)), dma((3,)), dma((2,)), dma((2, 2))] + Exchange.scratch(d))
    return pl.pallas_call(
        stack_kernel,
        in_specs=[any_spec(), vmem_spec(), pl.BlockSpec(memory_space=pltpu.SMEM)] + [vmem_spec()] * 2 + [any_spec()] * 4,
        out_specs=[any_spec()] * 11 + [vmem_spec()] * 2,
        out_shape=outs,
        scratch_shapes=scratch,
        compiler_params=pltpu.CompilerParams(collective_id=0, has_side_effects=True, vmem_limit_bytes=VMEM_LIMIT),
        name='stack',
    )(x, dy, lens, vec, bup, wqkv, wout, wup, wdown)


def wgrad_kernel(lhs_f, lhs_b, rhs_f, rhs_b, y_in, dx_in, bup_in, vec_in, g_up, g_down, g_qkv, g_out, y_out, dx_out, bup_out, vec_out,
                 lbuf, rbuf, obuf, lsem, rsem, osem, small_sem, *small_buf):
    small_in, small_out = (y_in, dx_in, bup_in, vec_in), (y_out, dx_out, bup_out, vec_out)
    n, rows, d = rhs_f.shape
    kinds = ((lhs_f, 0, TILE, d // TILE, rhs_b.at[0], g_up), (lhs_f, d, TILE, d // TILE, rhs_b.at[1], g_down),
             (lhs_b, 0, QKV // 2, 2, rhs_f, g_qkv), (lhs_f, 2 * d, HEADS, 1, rhs_b.at[2], g_out))
    base = [n * sum(k[3] for k in kinds[:i]) for i in range(len(kinds))]

    def lhs_copy(kind, s):
        src, first, tile, per, _, _ = kinds[kind]
        cols = pl.ds(pl.multiple_of(first + lax.rem(s, per) * tile, SEQ), tile)
        slot = lax.rem(base[kind] + s, 3)
        return pltpu.make_async_copy(src.at[s // per, :, cols], lbuf.at[slot, :, pl.ds(0, tile)], lsem.at[slot])

    def rhs_copy(kind, l):
        slot = lax.rem(l, 2)
        return pltpu.make_async_copy(kinds[kind][4].at[l], rbuf.at[slot], rsem.at[slot])

    def out_copy(kind, s):
        tile, per, out = kinds[kind][2], kinds[kind][3], kinds[kind][5]
        slot = lax.rem(s, 2)
        at = pl.ds(pl.multiple_of(lax.rem(s, per) * tile, SEQ), tile)
        return pltpu.make_async_copy(obuf.at[slot, pl.ds(0, tile)], out.at[s // per, at], osem.at[slot])

    loads = [pltpu.make_async_copy(src, buf, small_sem.at[i]) for i, (src, buf) in enumerate(zip(small_in, small_buf))]
    stores = [pltpu.make_async_copy(buf, dst, small_sem.at[i]) for i, (dst, buf) in enumerate(zip(small_out, small_buf))]
    rhs_copy(0, 0).start()
    lhs_copy(0, 0).start()
    lhs_copy(0, 1).start()
    for copy in loads:
        copy.start()
    for kind, (_, _, tile, per, _, _) in enumerate(kinds):
        steps = n * per

        @pl.loop(0, steps)
        def _(s):
            @pl.when(s + 2 < steps)
            def _():
                lhs_copy(kind, s + 2).start()

            @pl.when((lax.rem(s, per) == 0) & (s // per + 1 < n))
            def _():
                rhs_copy(kind, s // per + 1).start()

            if kind + 1 < len(kinds):
                @pl.when(s + 2 == steps)
                def _():
                    lhs_copy(kind + 1, 0).start()

                @pl.when(s + 1 == steps)
                def _():
                    lhs_copy(kind + 1, 1).start()
                    rhs_copy(kind + 1, 0).start()

            lhs_copy(kind, s).wait()

            @pl.when(lax.rem(s, per) == 0)
            def _():
                rhs_copy(kind, s // per).wait()

            @pl.when(s >= 2)
            def _():
                out_copy(kind, s - 2).wait()

            if kind > 0:
                @pl.when(s < 2)
                def _():
                    out_copy(kind - 1, n * kinds[kind - 1][3] - 2 + s).wait()

            lhs = lbuf[lax.rem(base[kind] + s, 3), :, pl.ds(0, tile)]
            obuf[lax.rem(s, 2), pl.ds(0, tile)] = dot_tn(lhs, rbuf[lax.rem(s // per, 2)]).astype(BF)
            out_copy(kind, s).start()

        if kind == 0:
            for load, store in zip(loads, stores):
                load.wait()
                store.start()

    last = n * kinds[-1][3]
    for s in (last - 2, last - 1):
        out_copy(len(kinds) - 1, s).wait()
    for copy in stores:
        copy.wait()


def weight_grads(lhs_f, lhs_b, rhs_f, rhs_b, *small):
    n, rows, d = rhs_f.shape
    widths = (d, d, lhs_b.shape[2], lhs_f.shape[2] - 2 * d)
    dma = pltpu.SemaphoreType.DMA
    return pl.pallas_call(
        wgrad_kernel,
        in_specs=[any_spec()] * 8,
        out_specs=[any_spec()] * 8,
        out_shape=[jax.ShapeDtypeStruct((n, w, d), BF) for w in widths] + [jax.ShapeDtypeStruct(v.shape, v.dtype) for v in small],
        scratch_shapes=[pltpu.VMEM((3, rows, TILE), BF), pltpu.VMEM((2, rows, d), BF), pltpu.VMEM((2, TILE, d), BF),
                        dma((3,)), dma((2,)), dma((2,)), dma((4,))] + [pltpu.VMEM(v.shape, v.dtype) for v in small],
        compiler_params=pltpu.CompilerParams(vmem_limit_bytes=VMEM_LIMIT),
        cost_estimate=pl.CostEstimate(flops=2 * n * rows * d * sum(widths), bytes_accessed=2 * n * d * sum(widths), transcendentals=0),
        name='weight_grads',
    )(lhs_f, lhs_b, rhs_f, rhs_b, *small)


def group_body(x_loc, dy_loc, len_loc, wqkv_loc, wout_loc, wup_loc, bup_loc, wdown_loc, vec_loc):
    n, d = wqkv_loc.shape[0], x_loc.shape[-1]
    vec = vec_loc.transpose(1, 0, 2)
    wqkv = wqkv_loc.transpose(0, 2, 3, 4, 1).reshape(n, QKV, d)
    wout = wout_loc.reshape(n, HEADS, d)
    outs = run_stack(x_loc, dy_loc, len_loc, vec, bup_loc, wqkv, wout, wup_loc, wdown_loc)
    y, d_x, _, _, a_s, _, _, _, lhs_s, dqkv_s, rhs_s, g_bup, g_vec = outs
    operands = (lhs_s.reshape(n, TOKENS, -1), dqkv_s.reshape(n, TOKENS, -1), a_s.reshape(n, TOKENS, d), rhs_s.reshape(3, n, TOKENS, d))
    g_up, g_down, g_qkv, g_out, y, d_x, g_bup, g_vec = weight_grads(*operands, y, d_x, g_bup, g_vec)
    g_qkv = g_qkv.reshape(n, 3, 8, HALF, d).transpose(0, 4, 1, 2, 3)
    g_out = g_out.reshape(n, 8, HALF, d)
    return y, d_x, g_qkv, g_out, g_up, g_bup, g_down, g_vec.transpose(1, 0, 2)


def solution(mesh):
    act_spec = P(PARTS_AXIS, TENSOR_AXIS, None)
    in_specs = (act_spec, act_spec, P(PARTS_AXIS), P(None, None, None, TENSOR_AXIS, None), P(None, TENSOR_AXIS, None, None), P(None, None, TENSOR_AXIS), P(None, TENSOR_AXIS), P(None, TENSOR_AXIS, None), P())
    out_specs = (act_spec, act_spec, P(PARTS_AXIS, None, None, TENSOR_AXIS, None), P(PARTS_AXIS, TENSOR_AXIS, None, None), P(PARTS_AXIS, None, TENSOR_AXIS), P(PARTS_AXIS, TENSOR_AXIS), P(PARTS_AXIS, TENSOR_AXIS, None), P(PARTS_AXIS, None, None))
    return jax.shard_map(group_body, mesh=mesh, in_specs=in_specs, out_specs=out_specs, check_vma=False)
```

```python
import functools
import jax
import jax.numpy as jnp
from jax import lax
from jax.experimental import pallas as pl
from jax.experimental.pallas import tpu as pltpu
from jax.sharding import PartitionSpec as P

TENSOR_AXIS = 'tp'
PARTS_AXIS = 'dp'
BF = jnp.bfloat16
F32 = jnp.float32
MESH = pl.DeviceIdType.MESH
VMEM_LIMIT = 67043328
SEQ = 128
HALF = 64
SHARD = 32
ROWS = 256
HEADS = 512
QKV = 3 * HEADS
TILE = 1024
BATCH = 4
TOKENS = BATCH * SEQ
OWN = pl.ds(0, SHARD)
NUM_CHUNKS = 2
RS_BLOCKS = 4
GELU_C = 0.7978845608028654


def dot_nn(a, b):
    return lax.dot_general(a, b, (((1,), (0,)), ((), ())), preferred_element_type=F32)


def dot_nt(a, b):
    return lax.dot_general(a, b, (((1,), (1,)), ((), ())), preferred_element_type=F32)


def dot_tn(a, b):
    return lax.dot_general(a, b, (((0,), (0,)), ((), ())), preferred_element_type=F32)


def seqs(c):
    return pl.ds(2 * c, 2)


def pair_of(c):
    return 2 * c, 2 * c + 1


def rows_of(ref, c):
    val = ref[seqs(c)]
    return val.reshape(ROWS, val.shape[-1])


def normed(z):
    mean = jnp.mean(z, axis=-1, keepdims=True)
    centered = z - mean
    var = jnp.mean(centered * centered, axis=-1, keepdims=True)
    rstd = lax.rsqrt(var + 1e-5)
    return centered * rstd, rstd


class Exchange:
    def __init__(self, part, from_core, far_send, far_recv, sems):
        self.me = lax.axis_index(TENSOR_AXIS)
        self.part, self.from_core = part, from_core
        self.far_send, self.far_recv = far_send, far_recv
        self.gs, self.gr, self.cs, self.cr, self.xs, self.xr = sems

    def remote(self, src, dst, send, recv, flip):
        return pltpu.make_async_remote_copy(
            src_ref=src, dst_ref=dst, send_sem=send, recv_sem=recv,
            device_id={TENSOR_AXIS: lax.bitwise_xor(self.me, flip)}, device_id_type=MESH)

    def barrier(self):
        sem = pltpu.get_barrier_semaphore()
        for flip in (1, 2):
            pl.semaphore_signal(sem, inc=1, device_id={TENSOR_AXIS: lax.bitwise_xor(self.me, flip)}, device_id_type=MESH)
        pl.semaphore_wait(sem, 2)

    def gather(self, buf, seq):
        return self.remote(buf.at[seq, pl.ds(0, HALF)], buf.at[seq, pl.ds(HALF, HALF)], self.gs.at[seq], self.gr.at[seq], 1)

    def gather_wait(self, buf, c):
        for s in range(2):
            self.gather(buf, 2 * c + s).wait()

    def cols(self, b):
        width = self.part.shape[-1] // RS_BLOCKS
        return pl.ds(pl.multiple_of(b * width, width), width)

    def core_copy(self, c, b):
        return self.remote(self.part.at[seqs(c), pl.ds(HALF, HALF), self.cols(b)], self.from_core.at[seqs(c), :, self.cols(b)],
                           self.cs.at[c, b], self.cr.at[c, b], 1)

    def far_copy(self, kind, c, b, full):
        rows = pl.ds(0, HALF) if full else pl.ds(SHARD, SHARD)
        return self.remote(self.far_send.at[seqs(c), rows, self.cols(b)], self.far_recv.at[kind, seqs(c), rows, self.cols(b)],
                           self.xs.at[kind, c, b], self.xr.at[kind, c, b], 2)

    def middle(self, kind, c, b, full=True):
        self.core_copy(c, b).wait_recv()
        near = self.part[seqs(c), pl.ds(0, HALF), self.cols(b)].astype(F32)
        self.far_send[seqs(c), :, self.cols(b)] = (near + self.from_core[seqs(c), :, self.cols(b)].astype(F32)).astype(BF)
        if isinstance(full, bool):
            self.far_copy(kind, c, b, full).start()
        else:
            @pl.when(full)
            def _():
                self.far_copy(kind, c, b, True).start()

            @pl.when(jnp.logical_not(full))
            def _():
                self.far_copy(kind, c, b, False).start()

    def arrive(self, kind, c, full=True):
        @pl.loop(0, RS_BLOCKS)
        def _(b):
            self.far_copy(kind, c, b, full).wait_recv()
            self.far_copy(kind, c, b, full).wait_send()
            self.core_copy(c, b).wait_send()

    def total(self, kind, seq, full=True):
        own, twin = OWN, pl.ds(SHARD, SHARD)
        pairs = ((own, twin), (twin, own)) if full else ((own, twin),)
        sums = [self.far_send[seq, here].astype(F32) + self.far_recv[kind, seq, there].astype(F32) for here, there in pairs]
        return jnp.concatenate([v.astype(BF).astype(F32) for v in sums], axis=0)

    @staticmethod
    def scratch(d):
        dma = pltpu.SemaphoreType.DMA
        return [pltpu.VMEM((BATCH, SEQ, d), BF), pltpu.VMEM((BATCH, HALF, d), BF), pltpu.VMEM((BATCH, HALF, d), BF), pltpu.VMEM((2, 4, HALF, d), BF),
                dma((4,)), dma((4,)), dma((2, RS_BLOCKS)), dma((2, RS_BLOCKS)), dma((2, 2, RS_BLOCKS)), dma((2, 2, RS_BLOCKS))]


LAST = RS_BLOCKS - 1


def partial_sum(ex, kind, c, block_of, full=True):
    @pl.loop(0, RS_BLOCKS)
    def _(b):
        cols = ex.cols(b)
        ex.part[seqs(c), :, cols] = block_of(cols).astype(BF).reshape(2, SEQ, -1)
        ex.core_copy(c, b).start()

        @pl.when(b > 0)
        def _():
            ex.middle(kind, c, b - 1, full)


def lane_low():
    return lax.broadcasted_iota(jnp.int32, (SEQ, SEQ), 1) < HALF


def two_heads(val, low):
    zero = jnp.zeros_like(val)
    return jnp.concatenate([jnp.where(low, val, zero), jnp.where(low, zero, val)], axis=0)


def stack_kernel(x_in, dy_in, lens, vec, bup, wqkv_h, wout_h, wup_h, wdown_h,
                 y_out, d_x, x_s, hid_s, a_s, qkv_s, p_s, slope_s, lhs_s, dqkv_s, rhs_s, g_bup, g_vec,
                 wq, wo, wu, wd, xbuf, hbuf, dcur, ag_a, ag_m, qkv, ctx, prob, slope, act, dqkv, dyfar, vacc, vfar, vlast,
                 wsem, ssem, isem, rsem, zsem, vsem, part, from_core, far_send, far_recv, *sems):
    n_layers = wqkv_h.shape[0]
    last = n_layers - 1
    ex = Exchange(part, from_core, far_send, far_recv, sems)

    d = x_in.shape[-1]

    def lhs_cols(start, width):
        return lhs_s.at[:, :, :, pl.ds(start, width)]

    def weight_copies(l, kind):
        pairs = ((wqkv_h, wq, 0), (wout_h, wo, 1)) if kind == 0 else ((wup_h, wu, 2), (wdown_h, wd, 3))
        return [pltpu.make_async_copy(src.at[l], dst, wsem.at[i]) for src, dst, i in pairs]

    def fwd_saves(l, c, kind):
        if kind == 0:
            pairs = ((xbuf, x_s, 0), (ag_a, a_s, 1), (qkv, qkv_s, 2), (ctx, lhs_cols(2 * d, HEADS), 3), (prob, p_s, 4))
        else:
            pairs = ((hbuf, hid_s, 5), (ag_m, lhs_cols(0, d), 6), (slope, slope_s, 7), (act, lhs_cols(d, d), 8))
        return [pltpu.make_async_copy(src.at[seqs(c)], dst.at[l, seqs(c)], ssem.at[c, i]) for src, dst, i in pairs]

    def norm_and_gather(src, l, c, row, buf, update=None):
        for seq in pair_of(c):
            if update is not None:
                update(seq)
            xhat, _ = normed(src[seq])
            val = xhat * vec[row, pl.ds(l, 1), :] + vec[row + 1, pl.ds(l, 1), :]
            buf[seq, pl.ds(0, HALF)] = val.astype(BF)
            ex.gather(buf, seq).start()

    def dy_copy(c):
        return ex.remote(dy_in.at[seqs(c)], dyfar.at[seqs(c)], isem.at[2, c], isem.at[3, c], 2)

    def first_copy(c):
        return ex.remote(xbuf.at[seqs(c), OWN], xbuf.at[seqs(c), pl.ds(SHARD, SHARD)], isem.at[0, c], isem.at[1, c], 2)

    def position(axis):
        i = lax.broadcasted_iota(jnp.int32, (ROWS, SEQ), axis) & 127
        block = ((i >> 6) & 1) | ((i >> 4) & 2)
        return ((block ^ ex.me) << 5) | (i & 31)

    def attention(c):
        a = rows_of(ag_a, c)
        for j in range(3):
            cols = pl.ds(HEADS * j, HEADS)
            qkv[seqs(c), :, cols] = dot_nt(a, wq[cols, :]).astype(BF).reshape(2, SEQ, HEADS)
        low = lane_low()

        @pl.loop(0, 2)
        def _(s):
            seq = 2 * c + s
            key_pos, query_pos = position(1), position(0)
            visible = (key_pos <= query_pos) & (key_pos < lens[seq])
            for pair in range(4):
                q, k, v = (qkv[seq, :, pl.ds(HEADS * t + SEQ * pair, SEQ)] for t in range(3))
                scores = dot_nt(two_heads(q, low), k) * 0.125
                scores = jnp.where(visible, scores, -1e30)
                e = jnp.exp(scores - jnp.max(scores, axis=-1, keepdims=True))
                p = e / jnp.sum(e, axis=-1, keepdims=True)
                prob[seq, pair] = p
                pb = p.astype(BF)
                both = jnp.concatenate([pb[:SEQ], pb[SEQ:]], axis=1)
                ctx[seq, :, pl.ds(SEQ * pair, SEQ)] = dot_nn(both, two_heads(v, low)).astype(BF)

    def mlp(l, c):
        m = rows_of(ag_m, c)

        @pl.loop(0, 4)
        def _(j):
            cols = pl.ds(pl.multiple_of(HEADS * j, HEADS), HEADS)
            pre = dot_nn(m, wu[:, cols]) + bup[pl.ds(l, 1), cols]
            sq = pre * pre
            t = jnp.tanh(GELU_C * (pre + 0.044715 * (sq * pre)))
            grad = 0.5 * (1.0 + t) + 0.5 * pre * (1.0 - t * t) * (GELU_C * (1.0 + 0.134145 * sq))
            slope[seqs(c), :, cols] = grad.reshape(2, SEQ, HEADS)
            act[seqs(c), :, cols] = (0.5 * pre * (1.0 + t)).astype(BF).reshape(2, SEQ, HEADS)

    def loads(l, kind):
        if kind == 0:
            whole = ((wqkv_h, wq, 0), (wout_h, wo, 1))
            saved = ((qkv_s, qkv, 1), (p_s, prob, 2))
        else:
            whole = ((wdown_h, wd, 3), (wup_h, wu, 2))
            saved = ((slope_s, slope, 0),)
        return ([pltpu.make_async_copy(src.at[l], dst, wsem.at[i]) for src, dst, i in whole]
                + [pltpu.make_async_copy(src.at[l], dst, rsem.at[i]) for src, dst, i in saved])

    def z_load(l, c, kind):
        return pltpu.make_async_copy((x_s, hid_s)[kind].at[l, seqs(c)], xbuf.at[seqs(c)], zsem.at[c])

    def bwd_saves(l, c, kind):
        pairs = ((ag_a, rhs_s.at[2], 0), (dqkv, dqkv_s, 1)) if kind == 0 else ((ag_m, rhs_s.at[1], 2), (act, rhs_s.at[0], 3))
        return [pltpu.make_async_copy(src.at[seqs(c)], dst.at[l, seqs(c)], ssem.at[c, i]) for src, dst, i in pairs]

    def send(src, seq, buf):
        buf[seq, pl.ds(0, HALF)] = src[seq].astype(BF)
        ex.gather(buf, seq).start()

    def norm_bwd_and_send(kind, c, gain, base, dst, buf):
        terms = []
        for seq in pair_of(c):
            d_z = ex.total(kind, seq)
            d_ln, d_gain = norm_bwd(xbuf[seq], d_z, gain)
            dst[seq] = base[seq] + d_ln
            send(dst, seq, buf)
            terms.append((d_gain, d_z))
        return [jnp.stack(pair) for pair in zip(*terms)]

    def y_copy(c):
        return pltpu.make_async_copy(hbuf.at[seqs(c), OWN], y_out.at[seqs(c)], isem.at[1, c])

    def dx_copy(c):
        return pltpu.make_async_copy(dcur.at[seqs(c), OWN], d_x.at[seqs(c)], isem.at[0, c])

    def row_sum(val):
        sums = [jnp.sum(val[:, SHARD * i:SHARD * i + SHARD].reshape(HALF, -1), axis=0, keepdims=True) for i in range(val.shape[1] // SHARD)]
        return sums[0] if len(sums) == 1 else sums[0] + sums[1]

    def add_row(i, l, c, val):
        row = (i, pl.ds(l, 1))
        total = row_sum(val)
        vacc[row] = total if c == 0 else vacc[row] + total

    def norm_bwd(z, d_z, gain):
        shape = z.shape
        z, d_z = z.reshape(-1, shape[-1]), d_z.reshape(-1, shape[-1])
        xhat, rstd = normed(z)
        g = d_z * gain
        g_mean = jnp.mean(g, axis=-1, keepdims=True)
        gx_mean = jnp.mean(g * xhat, axis=-1, keepdims=True)
        return (rstd * (g - g_mean - xhat * gx_mean)).reshape(shape), (d_z * xhat).reshape(shape)

    def mlp_bwd(l, c):
        d_mlp = rows_of(ag_m, c)

        @pl.loop(0, 4)
        def _(j):
            cols = pl.ds(pl.multiple_of(HEADS * j, HEADS), HEADS)
            d_act = dot_nt(d_mlp, wd[cols, :]).astype(BF).astype(F32)
            d_pre = d_act * slope[seqs(c), :, cols].reshape(ROWS, HEADS)
            total = jnp.sum(d_pre, axis=0, keepdims=True)
            g_bup[pl.ds(l, 1), cols] = total if c == 0 else g_bup[pl.ds(l, 1), cols] + total
            act[seqs(c), :, cols] = d_pre.astype(BF).reshape(2, SEQ, HEADS)

    def attention_bwd(c):
        ctx[seqs(c)] = dot_nt(rows_of(ag_a, c), wo[...]).astype(BF).reshape(2, SEQ, HEADS)
        low = lane_low()

        @pl.loop(0, 2)
        def _(s):
            seq = 2 * c + s
            for pair in range(4):
                q, k, v = (qkv[seq, :, pl.ds(HEADS * t + SEQ * pair, SEQ)] for t in range(3))
                d_c = two_heads(ctx[seq, :, pl.ds(SEQ * pair, SEQ)], low)
                p = prob[seq, pair]
                d_p = dot_nt(d_c, v).astype(BF).astype(F32)
                d_s = p * (d_p - jnp.sum(d_p * p, axis=-1, keepdims=True))
                d_s = (d_s * 0.125).astype(BF)
                both = jnp.concatenate([d_s[:SEQ], d_s[SEQ:]], axis=1)
                d_q = dot_nn(both, two_heads(k, low))
                d_k = dot_tn(d_s, two_heads(q, low))
                d_v = dot_tn(p.astype(BF), d_c)
                for t, val in enumerate((d_q, d_k, d_v)):
                    dqkv[seq, :, pl.ds(HEADS * t + SEQ * pair, SEQ)] = val.astype(BF)

    x_copies = [pltpu.make_async_copy(x_in.at[seqs(c)], xbuf.at[seqs(c), OWN], isem.at[2, c]) for c in range(NUM_CHUNKS)]
    for copy in x_copies:
        copy.start()
    for kind in range(2):
        for copy in weight_copies(0, kind):
            copy.start()
    ex.barrier()
    for c in range(NUM_CHUNKS):
        x_copies[c].wait()
        first_copy(c).start()

    @pl.loop(0, n_layers)
    def _(l):
        for c in range(NUM_CHUNKS):
            @pl.when(l == 0)
            def _():
                first_copy(c).wait()
                norm_and_gather(xbuf, l, c, 0, ag_a)

            @pl.when(l > 0)
            def _():
                def update(seq):
                    xbuf[seq] = hbuf[seq] + ex.total(1, seq) + vec[5, pl.ds(l - 1, 1), :]

                ex.arrive(1, c)
                norm_and_gather(xbuf, l, c, 0, ag_a, update)

            if c == 0:
                @pl.when(l > 0)
                def _():
                    ex.middle(1, 1, LAST)

                for copy in weight_copies(l, 0):
                    copy.wait()
            else:
                ex.middle(0, 0, LAST)
            ex.gather_wait(ag_a, c)
            attention(c)
            for copy in fwd_saves(l, c, 0):
                copy.start()
            lhs = rows_of(ctx, c)
            partial_sum(ex, 0, c, lambda cols: dot_nn(lhs, wo[:, cols]))

        @pl.when(l + 1 < n_layers)
        def _():
            for copy in weight_copies(l + 1, 0):
                copy.start()

        for c in range(NUM_CHUNKS):
            def update(seq):
                hbuf[seq] = xbuf[seq] + ex.total(0, seq) + vec[4, pl.ds(l, 1), :]

            ex.arrive(0, c)
            norm_and_gather(hbuf, l, c, 2, ag_m, update)
            if c == 0:
                ex.middle(0, 1, LAST)

                @pl.when(l == last)
                def _():
                    for other in range(NUM_CHUNKS):
                        dy_copy(other).start()

                for copy in weight_copies(l, 1):
                    copy.wait()
            else:
                ex.middle(1, 0, LAST, l + 1 < n_layers)
            ex.gather_wait(ag_m, c)
            mlp(l, c)
            for copy in fwd_saves(l, c, 1):
                copy.start()
            for copy in fwd_saves(l, c, 0):
                copy.wait()
            lhs = rows_of(act, c)
            if c == 1:
                for copy in fwd_saves(l, 0, 1):
                    copy.wait()
            partial_sum(ex, 1, c, lambda cols: dot_nn(lhs, wd[:, cols]), l + 1 < n_layers)

        @pl.when(l + 1 < n_layers)
        def _():
            for copy in weight_copies(l + 1, 1):
                copy.start()

        for copy in fwd_saves(l, 1, 1):
            copy.wait()

    ex.middle(1, 1, LAST, False)
    for c in range(NUM_CHUNKS):
        z_load(last, c, 1).start()
    dcur[:, OWN] = dy_in[...].astype(F32)

    @pl.loop(0, n_layers)
    def _(i):
        l = last - i

        for c in range(NUM_CHUNKS):
            @pl.when(i == 0)
            def _():
                dy_copy(c).wait()
                dcur[seqs(c), pl.ds(SHARD, SHARD)] = dyfar[seqs(c)].astype(F32)
                for seq in pair_of(c):
                    send(dcur, seq, ag_m)

            @pl.when(i > 0)
            def _():
                ex.arrive(1, c)
                z_load(l + 1, c, 0).wait()
                d_gain, d_in = norm_bwd_and_send(1, c, vec[0, pl.ds(l + 1, 1), :], hbuf, dcur, ag_m)
                z_load(l, c, 1).start()
                if c == 0:
                    ex.middle(1, 1, LAST)
                add_row(0, l + 1, c, d_gain)
                add_row(1, l + 1, c, d_in)

            if c == 1:
                ex.middle(0, 0, LAST)
            add_row(5, l, c, dcur[seqs(c)])
            if c == 0:
                @pl.when(i > 0)
                def _():
                    for copy in loads(l, 1):
                        copy.wait()

            ex.gather_wait(ag_m, c)
            mlp_bwd(l, c)
            for copy in bwd_saves(l, c, 1):
                copy.start()

            @pl.when(i > 0)
            def _():
                for copy in bwd_saves(l + 1, c, 0):
                    copy.wait()

            @pl.when(i == 0)
            def _():
                own = OWN
                ex.arrive(1, c, False)
                for seq in pair_of(c):
                    hbuf[seq, own] = hbuf[seq, own] + ex.total(1, seq, False) + vec[5, pl.ds(last, 1), :]
                y_copy(c).start()

            lhs = rows_of(act, c)
            partial_sum(ex, 0, c, lambda cols: dot_nt(lhs, wu[cols, :]))

        for c in range(NUM_CHUNKS):
            @pl.when(i == 0)
            def _():
                y_copy(c).wait()

            ex.arrive(0, c)
            z_load(l, c, 1).wait()
            d_gain, d_mid = norm_bwd_and_send(0, c, vec[2, pl.ds(l, 1), :], dcur, hbuf, ag_a)
            z_load(l, c, 0).start()
            if c == 0:
                ex.middle(0, 1, LAST)
            else:
                ex.middle(1, 0, LAST, l > 0)
            add_row(2, l, c, d_gain)
            add_row(3, l, c, d_mid)
            add_row(4, l, c, hbuf[seqs(c)])
            if c == 0:
                @pl.when(i > 0)
                def _():
                    for copy in loads(l, 0):
                        copy.wait()
            else:
                @pl.when(l > 0)
                def _():
                    for copy in loads(l - 1, 1):
                        copy.start()

            ex.gather_wait(ag_a, c)
            attention_bwd(c)
            for copy in bwd_saves(l, c, 0):
                copy.start()
            for copy in bwd_saves(l, c, 1):
                copy.wait()
            lhs = rows_of(dqkv, c)
            partial_sum(ex, 1, c, lambda cols: dot_nn(lhs, wq[:, cols]), l > 0)

        @pl.when(l > 0)
        def _():
            for copy in loads(l - 1, 0):
                copy.start()

    ex.middle(1, 1, LAST, False)
    for c in range(NUM_CHUNKS):
        z_load(0, c, 0).wait()
        for copy in bwd_saves(0, c, 0):
            copy.wait()
        ex.arrive(1, c, False)
        d_in = jnp.stack([ex.total(1, seq, False) for seq in pair_of(c)])
        d_ln, d_gain = norm_bwd(xbuf[seqs(c), OWN], d_in, vec[0, pl.ds(0, 1), :])
        dcur[seqs(c), OWN] = hbuf[seqs(c), OWN] + d_ln
        dx_copy(c).start()
        for row, val in enumerate((d_gain, d_in)):
            total = row_sum(val)
            at = (0, pl.ds(row, 1))
            vlast[at] = total if c == 0 else vlast[at] + total
    copy = ex.remote(vlast.at[0], vlast.at[1], vsem.at[0, 0], vsem.at[0, 1], 2)
    copy.start()
    copy.wait()
    for row in range(2):
        vacc[row, pl.ds(0, 1)] = vlast[0, pl.ds(row, 1)] + vlast[1, pl.ds(row, 1)]
    copy = ex.remote(vacc, vfar, vsem.at[1, 0], vsem.at[1, 1], 1)
    copy.start()
    copy.wait()
    g_vec[...] = vacc[...] + vfar[...]
    for c in range(NUM_CHUNKS):
        dx_copy(c).wait()


def any_spec():
    return pl.BlockSpec(memory_space=pl.ANY)


def vmem_spec():
    return pl.BlockSpec(memory_space=pltpu.VMEM)


def run_stack(x, dy, lens, vec, bup, wqkv, wout, wup, wdown):
    n, d = wqkv.shape[0], x.shape[-1]
    shape = jax.ShapeDtypeStruct
    vmem = pltpu.VMEM
    dma = pltpu.SemaphoreType.DMA
    own, held, tokens = (BATCH, SHARD, d), (BATCH, HALF, d), (BATCH, SEQ, d)
    qkv, prob = (BATCH, SEQ, QKV), (BATCH, BATCH, ROWS, SEQ)
    outs = ([shape(own, F32)] * 2 + [shape((n, *held), F32)] * 2
            + [shape((n, *tokens), BF), shape((n, *qkv), BF), shape((n, *prob), F32), shape((n, *tokens), F32), shape((n, BATCH, SEQ, 2 * d + HEADS), BF),
               shape((n, *qkv), BF), shape((3, n, *tokens), BF), shape((n, d), F32), shape((6, n, d), F32)])
    scratch = ([vmem((QKV, d), BF), vmem((HEADS, d), BF), vmem((d, d), BF), vmem((d, d), BF)] + [vmem(held, F32)] * 3 + [vmem(tokens, BF)] * 2
               + [vmem(qkv, BF), vmem((BATCH, SEQ, HEADS), BF), vmem(prob, F32), vmem(tokens, F32), vmem(tokens, BF), vmem(qkv, BF), vmem(own, BF)]
               + [vmem((6, n, d), F32)] * 2 + [vmem((2, 2, d), F32)]
               + [dma((4,)), dma((2, 9)), dma((4, 2)), dma((3,)), dma((2,)), dma((2, 2))] + Exchange.scratch(d))
    return pl.pallas_call(
        stack_kernel,
        in_specs=[any_spec(), vmem_spec(), pl.BlockSpec(memory_space=pltpu.SMEM)] + [vmem_spec()] * 2 + [any_spec()] * 4,
        out_specs=[any_spec()] * 11 + [vmem_spec()] * 2,
        out_shape=outs,
        scratch_shapes=scratch,
        compiler_params=pltpu.CompilerParams(collective_id=0, has_side_effects=True, vmem_limit_bytes=VMEM_LIMIT),
        name='stack',
    )(x, dy, lens, vec, bup, wqkv, wout, wup, wdown)


def wgrad_kernel(lhs_f, lhs_b, rhs_f, rhs_b, y_in, dx_in, bup_in, vec_in, g_up, g_down, g_qkv, g_out, y_out, dx_out, bup_out, vec_out,
                 lbuf, rbuf, obuf, lsem, rsem, osem, small_sem, *small_buf):
    small_in, small_out = (y_in, dx_in, bup_in, vec_in), (y_out, dx_out, bup_out, vec_out)
    n, rows, d = rhs_f.shape
    kinds = ((lhs_f, 0, TILE, d // TILE, rhs_b.at[0], g_up), (lhs_f, d, TILE, d // TILE, rhs_b.at[1], g_down),
             (lhs_b, 0, QKV // 2, 2, rhs_f, g_qkv), (lhs_f, 2 * d, HEADS, 1, rhs_b.at[2], g_out))
    base = [n * sum(k[3] for k in kinds[:i]) for i in range(len(kinds))]

    def lhs_copy(kind, s):
        src, first, tile, per, _, _ = kinds[kind]
        cols = pl.ds(pl.multiple_of(first + lax.rem(s, per) * tile, SEQ), tile)
        slot = lax.rem(base[kind] + s, 3)
        return pltpu.make_async_copy(src.at[s // per, :, cols], lbuf.at[slot, :, pl.ds(0, tile)], lsem.at[slot])

    def rhs_copy(kind, l):
        slot = lax.rem(l, 2)
        return pltpu.make_async_copy(kinds[kind][4].at[l], rbuf.at[slot], rsem.at[slot])

    def out_copy(kind, s):
        tile, per, out = kinds[kind][2], kinds[kind][3], kinds[kind][5]
        slot = lax.rem(s, 2)
        at = pl.ds(pl.multiple_of(lax.rem(s, per) * tile, SEQ), tile)
        return pltpu.make_async_copy(obuf.at[slot, pl.ds(0, tile)], out.at[s // per, at], osem.at[slot])

    loads = [pltpu.make_async_copy(src, buf, small_sem.at[i]) for i, (src, buf) in enumerate(zip(small_in, small_buf))]
    stores = [pltpu.make_async_copy(buf, dst, small_sem.at[i]) for i, (dst, buf) in enumerate(zip(small_out, small_buf))]
    rhs_copy(0, 0).start()
    lhs_copy(0, 0).start()
    lhs_copy(0, 1).start()
    for copy in loads:
        copy.start()
    for kind, (_, _, tile, per, _, _) in enumerate(kinds):
        steps = n * per

        @pl.loop(0, steps)
        def _(s):
            @pl.when(s + 2 < steps)
            def _():
                lhs_copy(kind, s + 2).start()

            @pl.when((lax.rem(s, per) == 0) & (s // per + 1 < n))
            def _():
                rhs_copy(kind, s // per + 1).start()

            if kind + 1 < len(kinds):
                @pl.when(s + 2 == steps)
                def _():
                    lhs_copy(kind + 1, 0).start()

                @pl.when(s + 1 == steps)
                def _():
                    lhs_copy(kind + 1, 1).start()
                    rhs_copy(kind + 1, 0).start()

            lhs_copy(kind, s).wait()

            @pl.when(lax.rem(s, per) == 0)
            def _():
                rhs_copy(kind, s // per).wait()

            @pl.when(s >= 2)
            def _():
                out_copy(kind, s - 2).wait()

            if kind > 0:
                @pl.when(s < 2)
                def _():
                    out_copy(kind - 1, n * kinds[kind - 1][3] - 2 + s).wait()

            lhs = lbuf[lax.rem(base[kind] + s, 3), :, pl.ds(0, tile)]
            obuf[lax.rem(s, 2), pl.ds(0, tile)] = dot_tn(lhs, rbuf[lax.rem(s // per, 2)]).astype(BF)
            out_copy(kind, s).start()

        if kind == 0:
            for load, store in zip(loads, stores):
                load.wait()
                store.start()

    last = n * kinds[-1][3]
    for s in (last - 2, last - 1):
        out_copy(len(kinds) - 1, s).wait()
    for copy in stores:
        copy.wait()


def weight_grads(lhs_f, lhs_b, rhs_f, rhs_b, *small):
    n, rows, d = rhs_f.shape
    widths = (d, d, lhs_b.shape[2], lhs_f.shape[2] - 2 * d)
    dma = pltpu.SemaphoreType.DMA
    return pl.pallas_call(
        wgrad_kernel,
        in_specs=[any_spec()] * 8,
        out_specs=[any_spec()] * 8,
        out_shape=[jax.ShapeDtypeStruct((n, w, d), BF) for w in widths] + [jax.ShapeDtypeStruct(v.shape, v.dtype) for v in small],
        scratch_shapes=[pltpu.VMEM((3, rows, TILE), BF), pltpu.VMEM((2, rows, d), BF), pltpu.VMEM((2, TILE, d), BF),
                        dma((3,)), dma((2,)), dma((2,)), dma((4,))] + [pltpu.VMEM(v.shape, v.dtype) for v in small],
        compiler_params=pltpu.CompilerParams(vmem_limit_bytes=VMEM_LIMIT),
        cost_estimate=pl.CostEstimate(flops=2 * n * rows * d * sum(widths), bytes_accessed=2 * n * d * sum(widths), transcendentals=0),
        name='weight_grads',
    )(lhs_f, lhs_b, rhs_f, rhs_b, *small)


def group_body(x_loc, dy_loc, len_loc, wqkv_loc, wout_loc, wup_loc, bup_loc, wdown_loc, vec_loc):
    n, d = wqkv_loc.shape[0], x_loc.shape[-1]
    vec = vec_loc.transpose(1, 0, 2)
    wqkv = wqkv_loc.transpose(0, 2, 3, 4, 1).reshape(n, QKV, d)
    wout = wout_loc.reshape(n, HEADS, d)
    outs = run_stack(x_loc, dy_loc, len_loc, vec, bup_loc, wqkv, wout, wup_loc, wdown_loc)
    y, d_x, _, _, a_s, _, _, _, lhs_s, dqkv_s, rhs_s, g_bup, g_vec = outs
    operands = (lhs_s.reshape(n, TOKENS, -1), dqkv_s.reshape(n, TOKENS, -1), a_s.reshape(n, TOKENS, d), rhs_s.reshape(3, n, TOKENS, d))
    g_up, g_down, g_qkv, g_out, y, d_x, g_bup, g_vec = weight_grads(*operands, y, d_x, g_bup, g_vec)
    g_qkv = g_qkv.reshape(n, 3, 8, HALF, d).transpose(0, 4, 1, 2, 3)
    g_out = g_out.reshape(n, 8, HALF, d)
    return y, d_x, g_qkv, g_out, g_up, g_bup, g_down, g_vec.transpose(1, 0, 2)


def solution(mesh):
    act_spec = P(PARTS_AXIS, TENSOR_AXIS, None)
    in_specs = (act_spec, act_spec, P(PARTS_AXIS), P(None, None, None, TENSOR_AXIS, None), P(None, TENSOR_AXIS, None, None), P(None, None, TENSOR_AXIS), P(None, TENSOR_AXIS), P(None, TENSOR_AXIS, None), P())
    out_specs = (act_spec, act_spec, P(PARTS_AXIS, None, None, TENSOR_AXIS, None), P(PARTS_AXIS, TENSOR_AXIS, None, None), P(PARTS_AXIS, None, TENSOR_AXIS), P(PARTS_AXIS, TENSOR_AXIS), P(PARTS_AXIS, TENSOR_AXIS, None), P(PARTS_AXIS, None, None))
    return jax.shard_map(group_body, mesh=mesh, in_specs=in_specs, out_specs=out_specs, check_vma=False)
```
